256 devices in a mesh: gx: 4 (over x), gy: 8 (over y, core), gz: 8 (over z).
Axes of the slice: x: 4, y: 4, z: 8, core: 2. Of those that a mesh axis runs over, the one named last changes fastest.
Arguments:
- queries: bfloat16 [16384, 4096], P(('gx', 'gy'), 'gz'), may hold values from -6 to 6
- key_rows: bfloat16 [16384, 4096], P(('gx', 'gy'), 'gz'), may hold values from -24 to 24
- values: bfloat16 [16384, 4096], P(('gx', 'gy'), 'gz'), may hold values from -24 to 24
- tile_list: int32 [64, 32, 8], P(('gx', 'gy'), 'gz'), may hold values from 0 to 63, as said below
- out_weight: bfloat16 [4096, 4096], P('gz'), may hold values from -0.09375 to 0.09375
Outputs:
- projected: bfloat16 [16384, 4096], P(('gx', 'gy', 'gz'))
The draws below stay inside these ranges and needn't reach their ends.
Inputs may be any that keep to these rules, and one draw needn't show every extreme that they name: `tile_list`: each (query block, head) lists 8 different key blocks, one of which is the query block itself.
All inputs are finite; a program needn't handle non-finite values.
Results may differ from the reference program's by a relative error of at most 0.012.
Values may be sent and summed in bfloat16 or wider, within the bound.
No kernel may reach another device: no remote copies, remote signals or barrier semaphores. Data moves between devices by JAX's collectives and lax.ppermute only.
A program may use at most 64 MiB of HBM per device.

```python
import jax
import jax.numpy as jnp
from jax import lax

HEADS = 32
HD = 128
D = 4096
BLOCK = 256
TILES = 8
BLOCKS_PER_SHARD = 2
TOTAL_BLOCKS = 64
SEQ = 16384


def draw_key_rows(key, part):
    key_base, key_row, key_col = jax.random.split(key, 3)
    width_all = HEADS * HD
    normal_part = jnp.clip(jax.random.normal(key_base, (SEQ, width_all), jnp.float32), -4.0, 4.0)
    row_scale = jnp.exp(jax.random.uniform(key_row, (SEQ, 1), jnp.float32, -1.15, 1.15))
    col_scale = jnp.exp(jax.random.uniform(key_col, (1, width_all), jnp.float32, -0.8, 0.8))
    return jnp.clip(normal_part * row_scale * col_scale, -24.0, 24.0).astype(jnp.bfloat16)


def draw_tile_list(key, part):
    shard_of_keys, key_score = jax.random.split(jax.random.fold_in(key, 7), 2)
    local_shard_boost = jax.random.randint(shard_of_keys, (TOTAL_BLOCKS // BLOCKS_PER_SHARD,), 0, 3)
    block_numbers = jnp.arange(TOTAL_BLOCKS, dtype=jnp.int32)
    score_boost = local_shard_boost[block_numbers // BLOCKS_PER_SHARD]
    block_scores = jax.random.randint(key_score, (TOTAL_BLOCKS, HEADS, TOTAL_BLOCKS), 0, 4 * TOTAL_BLOCKS)
    block_scores = block_scores + score_boost[None, None, :] * TOTAL_BLOCKS
    own = (block_numbers[:, None, None] == block_numbers[None, None, :]).astype(jnp.int32)
    block_scores = block_scores + own * (64 * TOTAL_BLOCKS)
    block_scores = block_scores * TOTAL_BLOCKS + block_numbers[None, None, :]
    picked = jax.lax.top_k(block_scores, TILES)[1]
    return picked.astype(jnp.int32)


def steps_of(key, shape, cuts, least, largest):
    def one(dim, parts):
        heights = jax.random.uniform(jax.random.fold_in(jax.random.fold_in(key, 6), dim), (parts,), jnp.float32, least / len(cuts), largest / len(cuts))
        return jnp.repeat(jnp.exp(heights), shape[dim] // parts).reshape((-1,) + (1,) * (len(shape) - dim - 1))

    gain = one(*cuts[0])
    for cut in cuts[1:]:
        gain = gain * one(*cut)
    return gain


def gaussian(own_key, extent, spread, most, shards=(), held_as=jnp.bfloat16):
    result = spread * jax.random.normal(own_key, extent, jnp.float32)
    if shards:
        result = result * steps_of(own_key, extent, shards, -0.22, 0.18)
    return jnp.clip(result, -most, most).astype(held_as)


def setup_inputs(seed: int = 0) -> dict:
    keys = jax.random.split(jax.random.key(seed), 6)
    queries = gaussian(keys[0], (SEQ, HEADS * HD), 1.0, 6.0, ((0, 32), (1, 8)))
    key_rows = draw_key_rows(jax.random.fold_in(keys[5], 71), 0)
    values = gaussian(keys[2], (SEQ, HEADS * HD), 4.0, 24.0, ((0, 32), (1, 8)))
    tile_list = draw_tile_list(jax.random.fold_in(keys[5], 71), 0)
    out_weight = gaussian(keys[4], (HEADS * HD, D), (HEADS * HD) ** -0.5, 0.09375, ((0, 8),))
    return {"queries": queries, "key_rows": key_rows, "values": values, "tile_list": tile_list, "out_weight": out_weight}


def features(source):
    widened = source.astype(jnp.float32)
    return jnp.where(widened > 0, widened + 1.0, jnp.exp(jnp.minimum(widened, 0.0))).astype(jnp.bfloat16)


def reference(queries, key_rows, values, tile_list, out_weight):
    total = queries.shape[0]
    block_count = total // BLOCK
    query_feat = features(queries).reshape(block_count, BLOCK, HEADS, HD)
    key_feat = features(key_rows).reshape(block_count, BLOCK, HEADS, HD)
    value_rows = values.reshape(block_count, BLOCK, HEADS, HD)
    block_numbers = jnp.arange(block_count).astype(jnp.int32)

    def one_head(head_index):
        query_head = lax.dynamic_index_in_dim(query_feat, head_index, 2, keepdims=False).astype(jnp.float32)
        key_head = lax.dynamic_index_in_dim(key_feat, head_index, 2, keepdims=False).astype(jnp.float32)
        value_head = lax.dynamic_index_in_dim(value_rows, head_index, 2, keepdims=False).astype(jnp.float32)
        states = jnp.einsum('brd,bre->bde', key_head, value_head, precision=lax.Precision.HIGHEST).astype(jnp.bfloat16)
        key_sums = jnp.sum(key_head, axis=1)
        listed = lax.dynamic_index_in_dim(tile_list, head_index, 1, keepdims=False)
        chosen = jnp.sum((listed[:, :, None] == block_numbers[None, None, :]).astype(jnp.float32), axis=1)
        state_sums = jnp.dot(chosen.astype(jnp.bfloat16), states.reshape(block_count, HD * HD), preferred_element_type=jnp.float32)
        state_sums = state_sums.astype(jnp.bfloat16).reshape(block_count, HD, HD)
        norm_sums = jnp.dot(chosen, key_sums, precision=lax.Precision.HIGHEST)
        numerator = jnp.einsum('brd,bde->bre', query_head, state_sums.astype(jnp.float32), precision=lax.Precision.HIGHEST)
        denominator = jnp.einsum('brd,bd->br', query_head, norm_sums, precision=lax.Precision.HIGHEST)
        return (numerator / denominator[:, :, None]).astype(jnp.bfloat16).reshape(total, HD)

    attended = lax.map(one_head, jnp.arange(HEADS).astype(jnp.int32))
    attended = jnp.transpose(attended, (1, 0, 2)).reshape(total, HEADS * HD)
    return jnp.dot(attended, out_weight, preferred_element_type=jnp.float32).astype(jnp.bfloat16)
```

```python
import functools

import jax
import jax.numpy as jnp
from jax import lax
from jax.experimental import pallas as pl
from jax.experimental.pallas import tpu as pltpu
from jax.sharding import PartitionSpec as P

BLOCK = 256
HD = 128
UNIT = 144
STREAMS = 2
F32 = jnp.float32
BF16 = jnp.bfloat16


def call(kernel, out_shape, flops, vmem_mib, name):
    return pl.pallas_call(
        kernel,
        out_shape=out_shape,
        compiler_params=pltpu.CompilerParams(vmem_limit_bytes=vmem_mib << 20),
        cost_estimate=pl.CostEstimate(flops=flops, bytes_accessed=flops // 256, transcendentals=0),
        name=name,
    )


def features(source):
    widened = source.astype(F32)
    return jnp.where(widened > 0, widened + 1.0, jnp.exp(jnp.minimum(widened, 0.0))).astype(BF16)


def split_high_low(total):
    high = total.astype(BF16).astype(F32)
    return high, total - high


def states_kernel(k_ref, v_ref, lists_ref, ua_ref, ub_ref):
    row = lax.broadcasted_iota(jnp.int32, (16, HD), 0)
    ones = jnp.ones((16, BLOCK), BF16)
    for half, (u_ref, other_ref) in enumerate(((ua_ref, ub_ref), (ub_ref, ua_ref))):
        for b in range(2):
            for hh in range(2):
                h = 2 * half + hh
                at = (b * 2 + hh) * UNIT
                kf = features(k_ref[b * BLOCK : (b + 1) * BLOCK, h * HD : (h + 1) * HD])
                v = v_ref[b * BLOCK : (b + 1) * BLOCK, h * HD : (h + 1) * HD]
                state = lax.dot_general(v, kf, (((0,), (0,)), ((), ())), preferred_element_type=F32)
                u_ref[at : at + HD, :] = state.astype(BF16)
                high, low = split_high_low(jnp.dot(ones, kf, preferred_element_type=F32))
                h_other = 2 * (1 - half) + hh
                listed = lists_ref[b * 4 + h_other : b * 4 + h_other + 1, :]
                extra = jnp.where(
                    row == 0, high, jnp.where(row == 1, listed, jnp.where(row == 2, low, 0.0))
                )
                u_ref[at + HD : at + UNIT, :] = extra.astype(BF16)


def partial_kernel(kb_ref, *refs):
    own = (refs[0:4], refs[4:8])
    mate = (refs[8:12], refs[12:16])
    outs = (refs[16:20], refs[20:24])
    lane = lax.broadcasted_iota(jnp.int32, (HD, 256), 0)
    col = lax.broadcasted_iota(jnp.int32, (HD, 256), 1)
    spread = jnp.where(lax.rem(lane, 16) == col // 16, 1.0, 0.0).astype(BF16)
    same = jnp.where(lax.rem(lane, 16) == lax.rem(col, 16), 1.0, 0.0)
    row = lax.broadcasted_iota(jnp.int32, (16, HD), 0)
    for half in range(2):
        kb = kb_ref[half : half + 1, :]
        for hh in range(2):
            rows = []
            for d in range(4):
                for b in range(2):
                    at = (b * 2 + hh) * UNIT + HD
                    tile = own[1 - half][d][at : at + 16, :].astype(F32)
                    rows.append(jnp.broadcast_to(tile[1:2, :], (16, HD)))
            hit = jnp.where(jnp.concatenate(rows, axis=0) == kb, 1.0, 0.0).astype(BF16)
            chosen = jnp.dot(hit, spread, preferred_element_type=F32)
            mix = (chosen * same).astype(BF16)
            for g in range(9):
                pieces = []
                for d in range(4):
                    for side in (own, mate):
                        for b in range(2):
                            at = (b * 2 + hh) * UNIT + g * 16
                            pieces.append(side[half][d][at : at + 16, :])
                summed = jnp.dot(mix, jnp.concatenate(pieces, axis=0), preferred_element_type=F32)
                for d in range(4):
                    for b in range(2):
                        at = (b * 2 + hh) * UNIT + g * 16
                        piece = summed[(d * 2 + b) * 16 : (d * 2 + b + 1) * 16, :]
                        if g == 8:
                            high, low = split_high_low(piece[0:1, :] + piece[2:3, :])
                            piece = jnp.where(row == 0, high, jnp.where(row == 2, low, 0.0))
                        outs[half][d][at : at + 16, :] = piece.astype(BF16)


def attend_kernel(at_ref, qf_ref, w_ref, *refs):
    parts = (refs[0:4], refs[4:8])
    att_ref = refs[8]
    sends = refs[9:]
    for half in range(2):
        for b in range(2):
            for hh in range(2):
                h = 2 * half + hh
                at = (b * 2 + hh) * UNIT
                total = sum(p[at : at + UNIT, :].astype(F32) for p in parts[half])
                state = total[:HD].astype(BF16)
                high, low = split_high_low(total[HD : HD + 1] + total[HD + 2 : HD + 3])
                q = qf_ref[b * BLOCK : (b + 1) * BLOCK, h * HD : (h + 1) * HD]
                dims = (((1,), (1,)), ((), ()))
                num = lax.dot_general(q, state, dims, preferred_element_type=F32)
                den = lax.dot_general(
                    q, jnp.broadcast_to(high, (HD, HD)).astype(BF16), dims, preferred_element_type=F32
                ) + lax.dot_general(
                    q, jnp.broadcast_to(low, (HD, HD)).astype(BF16), dims, preferred_element_type=F32
                )
                att_ref[b * BLOCK : (b + 1) * BLOCK, h * HD : (h + 1) * HD] = (num / den).astype(BF16)
    far = att_ref[pl.ds(pl.multiple_of(at_ref[0] * 64, 64), 64), :]
    width = sends[0].shape[1]
    for i, send in enumerate(sends):
        send[...] = jnp.dot(
            far, w_ref[:, i * width : (i + 1) * width], preferred_element_type=F32
        ).astype(BF16)


def project_kernel(att_ref, w_ref, *t_refs):
    width = t_refs[0].shape[1]
    for s, t_ref in enumerate(t_refs):
        for c in range(0, width, 512):
            t_ref[:, c : c + 512] = jnp.dot(
                att_ref[...], w_ref[:, s * width + c : s * width + c + 512], preferred_element_type=F32
            )


def first_step_kernel(at_ref, t_ref, from_left_ref, from_right_ref, right_ref, left_ref):
    half = t_ref.shape[1] // 2
    right = pl.ds(pl.multiple_of(at_ref[0] * 64, 64), 64)
    left = pl.ds(pl.multiple_of(at_ref[1] * 64, 64), 64)
    right_ref[:, :half] = t_ref[right, :half].astype(BF16)
    right_ref[:, half:] = (t_ref[right, half:] + from_left_ref[...].astype(F32)).astype(BF16)
    left_ref[:, half:] = t_ref[left, half:].astype(BF16)
    left_ref[:, :half] = (t_ref[left, :half] + from_right_ref[...].astype(F32)).astype(BF16)


def step_kernel(at_ref, t_ref, from_left_ref, from_right_ref, right_ref, left_ref):
    right = pl.ds(pl.multiple_of(at_ref[0] * 64, 64), 64)
    left = pl.ds(pl.multiple_of(at_ref[1] * 64, 64), 64)
    right_ref[...] = (t_ref[right, :] + from_left_ref[...].astype(F32)).astype(BF16)
    left_ref[...] = (t_ref[left, :] + from_right_ref[...].astype(F32)).astype(BF16)


def last_kernel(at_ref, *refs):
    out_ref = refs[-1]
    own = pl.ds(pl.multiple_of(at_ref[0] * 64, 64), 64)
    for s in range(STREAMS):
        t_ref, from_left_ref, from_right_ref = refs[3 * s : 3 * s + 3]
        width = t_ref.shape[1]
        out_ref[:, s * width : (s + 1) * width] = (
            t_ref[own, :] + from_left_ref[...].astype(F32) + from_right_ref[...].astype(F32)
        ).astype(BF16)


def smem_call(kernel, out_shape, in_count, flops, vmem_mib, name):
    return pl.pallas_call(
        kernel,
        out_shape=out_shape,
        in_specs=[pl.BlockSpec(memory_space=pltpu.SMEM)]
        + [pl.BlockSpec(memory_space=pltpu.VMEM)] * (in_count - 1),
        compiler_params=pltpu.CompilerParams(vmem_limit_bytes=vmem_mib << 20),
        cost_estimate=pl.CostEstimate(flops=flops, bytes_accessed=flops // 256, transcendentals=0),
        name=name,
    )


def per_device(queries, key_rows, values, tile_list, out_weight):
    gx, gy, gz = (lax.axis_index(a) for a in ("gx", "gy", "gz"))
    y, core = gy // 2, gy % 2
    along_x = lambda a, d: lax.ppermute(a, "gx", [(i, (i + d) % 4) for i in range(4)])
    along_y = lambda a, d: lax.ppermute(
        a, "gy", [(i * 2 + c, (i + d) % 4 * 2 + c) for i in range(4) for c in range(2)]
    )
    to_mate = lambda a: lax.ppermute(a, "gy", [(i, i ^ 1) for i in range(8)])
    along_z = lambda a, d: lax.ppermute(a, "gz", [(i, (i + d) % 8) for i in range(8)])

    lists = jnp.repeat(tile_list.reshape(8, 8), 16, axis=1).astype(F32)
    k = lax.iota(jnp.int32, HD) % 16
    back, other, b = k // 4, k // 2 % 2, k % 2
    key_core = jnp.where(other == 1, 1 - core, core)
    blocks_a = 2 * (gx * 8 + (y - back) % 4 * 2 + key_core) + b
    blocks_b = 2 * ((gx - back) % 4 * 8 + y * 2 + key_core) + b
    key_blocks = jnp.stack([blocks_a, blocks_b]).astype(F32)

    unit = jax.ShapeDtypeStruct((4 * UNIT, HD), BF16)
    ua, ub = call(states_kernel, (unit, unit), 10**9, 8, "states")(key_rows, values, lists)
    own_a = [ua] + [along_y(ua, d) for d in (1, 2, 3)]
    own_b = [ub] + [along_x(ub, d) for d in (1, 2, 3)]
    mate_a = [to_mate(u) for u in own_a]
    mate_b = [to_mate(u) for u in own_b]
    parts = call(partial_kernel, (unit,) * 8, 10**9, 16, "partial")(
        key_blocks, *own_a, *own_b, *mate_a, *mate_b
    )
    parts_a, parts_b = parts[:4], parts[4:]
    got_a = [parts_a[0]] + [along_x(parts_a[d], -d) for d in (1, 2, 3)]
    got_b = [parts_b[0]] + [along_y(parts_b[d], -d) for d in (1, 2, 3)]

    qf = features(queries)
    width = out_weight.shape[1] // STREAMS
    far = jax.ShapeDtypeStruct((64, width // 2), BF16)
    att, *sends = smem_call(
        attend_kernel,
        (jax.ShapeDtypeStruct(queries.shape, BF16),) + (far,) * (2 * STREAMS),
        11,
        10**9,
        16,
        "attend",
    )(((gz + 4) % 8).reshape(1), qf, out_weight, *got_a, *got_b)
    streams = []
    for s in range(STREAMS):
        streams.append((along_z(sends[2 * s + 1], 1), along_z(sends[2 * s], -1)))
    ts = call(
        project_kernel,
        (jax.ShapeDtypeStruct((queries.shape[0], width), F32),) * STREAMS,
        4 * 10**9,
        20,
        "project",
    )(att, out_weight)
    piece = jax.ShapeDtypeStruct((64, width), BF16)
    for hop in (3, 2, 1):
        at = jnp.stack([(gz + hop) % 8, (gz - hop) % 8])
        kernel = first_step_kernel if hop == 3 else step_kernel
        for s in range(STREAMS):
            right, left = smem_call(kernel, (piece, piece), 4, 10**8, 6, f"hop{hop}")(
                at, ts[s], *streams[s]
            )
            streams[s] = (along_z(right, 1), along_z(left, -1))
    flat = [a for s in range(STREAMS) for a in (ts[s], *streams[s])]
    return smem_call(
        last_kernel,
        jax.ShapeDtypeStruct((64, out_weight.shape[1]), BF16),
        1 + len(flat),
        10**8,
        12,
        "last",
    )(gz.reshape(1), *flat)


def solution(mesh):
    return jax.shard_map(
        per_device,
        mesh=mesh,
        in_specs=(
            P(("gx", "gy"), "gz"),
            P(("gx", "gy"), "gz"),
            P(("gx", "gy"), "gz"),
            P(("gx", "gy"), "gz", None),
            P("gz", None),
        ),
        out_specs=P(("gx", "gy", "gz"), None),
        check_vma=False,
    )
```

```python
import jax
import jax.numpy as jnp
from jax import lax
from jax.experimental import pallas as pl
from jax.experimental.pallas import tpu as pltpu
from jax.sharding import PartitionSpec as P

BLOCK = 256
HD = 128
UNIT = 144
ROWS = 4 * UNIT
F32 = jnp.float32
BF16 = jnp.bfloat16


def call(kernel, out_shape, flops, vmem_mib, name):
    return pl.pallas_call(
        kernel,
        out_shape=out_shape,
        compiler_params=pltpu.CompilerParams(vmem_limit_bytes=vmem_mib << 20),
        cost_estimate=pl.CostEstimate(flops=flops, bytes_accessed=flops // 256, transcendentals=0),
        name=name,
    )


def features(source):
    widened = source.astype(F32)
    return jnp.where(widened > 0, widened + 1.0, jnp.exp(jnp.minimum(widened, 0.0))).astype(BF16)


def high_and_low(total):
    high = total.astype(BF16).astype(F32)
    row = lax.broadcasted_iota(jnp.int32, (16, HD), 0)
    return jnp.where(row == 0, high, jnp.where(row == 1, total - high, 0.0)).astype(BF16)


def head_columns(h):
    return pl.ds(pl.multiple_of(h * HD, HD), HD)


def chunk_rows(j):
    return pl.ds(pl.multiple_of(j * 64, 64), 64)


def states_kernel(k_hbm, v_hbm, keep_ref, send_ref, k_ref, v_ref, sems):
    copies = [
        pltpu.make_async_copy(hbm.at[rows], ref.at[rows], sems.at[i, b])
        for b, rows in enumerate((pl.ds(0, BLOCK), pl.ds(BLOCK, BLOCK)))
        for i, (hbm, ref) in enumerate(((k_hbm, k_ref), (v_hbm, v_ref)))
    ]
    for copy in copies:
        copy.start()
    core = lax.rem(lax.axis_index("gy"), 2)
    ones = jnp.ones((16, BLOCK), BF16)
    for b in range(2):
        rows = pl.ds(b * BLOCK, BLOCK)
        copies[2 * b].wait()
        copies[2 * b + 1].wait()
        for u_ref, role in ((keep_ref, core), (send_ref, 1 - core)):
            for hh in range(2):
                at = (b * 2 + hh) * UNIT
                columns = head_columns(2 * role + hh)
                kf = features(k_ref[rows, columns])
                state = lax.dot_general(
                    v_ref[rows, columns], kf, (((0,), (0,)), ((), ())), preferred_element_type=F32
                )
                u_ref[at : at + HD, :] = state.astype(BF16)
                total = jnp.dot(ones, kf, preferred_element_type=F32)
                u_ref[at + HD : at + UNIT, :] = high_and_low(total)


def partial_kernel(kb_ref, list_ref, *refs):
    keys, outs = refs[:8], refs[8:]
    lane = lax.broadcasted_iota(jnp.int32, (HD, 256), 0)
    col = lax.broadcasted_iota(jnp.int32, (HD, 256), 1)
    spread = jnp.where(lax.rem(lane, 16) == col // 16, 1.0, 0.0).astype(BF16)
    row = lax.broadcasted_iota(jnp.int32, (256, 256), 0)
    col = lax.broadcasted_iota(jnp.int32, (256, 256), 1)
    same = jnp.where(lax.rem(row, 16) == lax.rem(col, 16), 1.0, 0.0)
    blocks = [(d * 2 + c, b * 2 * UNIT) for d in range(4) for c in range(2) for b in range(2)]
    for hh in range(2):
        listed = [
            jnp.broadcast_to(list_ref[hh * 16 + q : hh * 16 + q + 1, :], (16, HD)) for q in range(16)
        ]
        hit = jnp.where(jnp.concatenate(listed, axis=0) == kb_ref[...], 1.0, 0.0).astype(BF16)
        mix = (jnp.dot(hit, spread, preferred_element_type=F32) * same).astype(BF16)
        for g in range(9):
            shift = hh * UNIT + g * 16
            pieces = [keys[d][at + shift : at + shift + 16, :] for d, at in blocks]
            summed = jnp.dot(mix, jnp.concatenate(pieces, axis=0), preferred_element_type=F32)
            for q, (d, at) in enumerate(blocks):
                piece = summed[q * 16 : q * 16 + 16, :]
                if g == 8:
                    outs[d][at + shift : at + shift + 16, :] = high_and_low(piece[0:1] + piece[1:2])
                else:
                    outs[d][at + shift : at + shift + 16, :] = piece.astype(BF16)


def attend(q_ref, state_ref, sums_ref, at, rows, columns):
    dims = (((1,), (1,)), ((), ()))
    q = q_ref[rows, columns]
    num = lax.dot_general(q, state_ref[at, :], dims, preferred_element_type=F32)
    sums = sums_ref[at, :]
    return (num / lax.dot_general(q, sums, dims, preferred_element_type=F32)).astype(BF16)


def far_kernel(qf_ref, w_ref, *refs):
    parts, (right_ref, left_ref, state_ref, sums_ref, att_ref) = (refs[:4], refs[4:8]), refs[8:]
    core, far = lax.rem(lax.axis_index("gy"), 2), lax.rem(lax.axis_index("gz") + 4, 8)
    for side in range(2):
        role = core if side == 0 else 1 - core
        for u in range(4):
            at = u * UNIT
            total = sum(p[at : at + UNIT, :].astype(F32) for p in parts[side])
            to = pl.ds(pl.multiple_of((u // 2 * 4 + 2 * role + u % 2) * HD, HD), HD)
            state_ref[to, :] = total[:HD].astype(BF16)
            key_sum = total[HD : HD + 1] + total[HD + 1 : HD + 2]
            sums_ref[to, :] = jnp.broadcast_to(key_sum, (HD, HD)).astype(BF16)
    for h in range(4):
        at = pl.ds(pl.multiple_of((far // 4 * 4 + h) * HD, HD), HD)
        columns = slice(h * HD, (h + 1) * HD)
        att_ref[:, columns] = attend(qf_ref, state_ref, sums_ref, at, chunk_rows(far), columns)
    half = w_ref.shape[1] // 2
    right_ref[...] = jnp.dot(att_ref[...], w_ref[:, half:], preferred_element_type=F32).astype(BF16)
    left_ref[...] = jnp.dot(att_ref[...], w_ref[:, :half], preferred_element_type=F32).astype(BF16)


def project_kernel(qf_ref, w_ref, state_ref, sums_ref, *refs):
    r3_ref, l3_ref, f3_ref, e2_ref, f2_ref, e1_ref, f1_ref, own_ref, att_ref = refs
    gz = lax.axis_index("gz")
    for b in range(2):
        for h in range(4):
            at, columns = pl.ds((b * 4 + h) * HD, HD), slice(h * HD, (h + 1) * HD)
            rows = pl.ds(b * BLOCK, BLOCK)
            att_ref[rows, columns] = attend(qf_ref, state_ref, sums_ref, at, rows, columns)
    hops = (3, 5, 2, 6, 1, 7, 0)
    lhs = jnp.concatenate([att_ref[chunk_rows(lax.rem(gz + hop, 8)), :] for hop in hops], axis=0)
    half = w_ref.shape[1] // 2
    for i in range(2):
        for c in range(0, half, 512):
            out = jnp.dot(lhs, w_ref[:, i * half + c : i * half + c + 512], preferred_element_type=F32)
            cols = slice(c, c + 512)
            for n, (e_ref, f_ref) in enumerate(((None, f3_ref), (e2_ref, f2_ref), (e1_ref, f1_ref))):
                right, left = out[n * 128 : n * 128 + 64], out[n * 128 + 64 : n * 128 + 128]
                early = (right, left)[i]
                f_ref[(64, 0)[i] : (128, 64)[i], cols] = (left, right)[i]
                if e_ref is None:
                    (r3_ref, l3_ref)[i][:, cols] = early.astype(BF16)
                else:
                    e_ref[(0, 64)[i] : (64, 128)[i], cols] = early
            own_ref[:, i * half + c : i * half + c + 512] = out[384:448]


def hop_kernel(term_ref, from_left_ref, from_right_ref, right_ref, left_ref):
    right_ref[...] = (term_ref[:64, :] + from_left_ref[...].astype(F32)).astype(BF16)
    left_ref[...] = (term_ref[64:, :] + from_right_ref[...].astype(F32)).astype(BF16)


def last_kernel(own_ref, right0, left1, right1, left0, out_ref):
    half = own_ref.shape[1] // 2
    for i, (a, b) in enumerate(((right0, left0), (right1, left1))):
        out_ref[:, i * half : (i + 1) * half] = (
            own_ref[:, i * half : (i + 1) * half] + a[...].astype(F32) + b[...].astype(F32)
        ).astype(BF16)


def per_device(queries, key_rows, values, tile_list, out_weight):
    gx, gy = lax.axis_index("gx"), lax.axis_index("gy")
    y, core = gy // 2, gy % 2

    def by_role(a, d, axes, cross=False):
        pairs = []
        for i in range(4):
            for j in range(4):
                for c in range(2):
                    to = ((i + d) % 4, j) if axes[c] == "x" else (i, (j + d) % 4)
                    pairs.append((i * 8 + j * 2 + c, to[0] * 8 + to[1] * 2 + (c ^ cross)))
        return lax.ppermute(a, ("gx", "gy"), pairs)

    to_mate = lambda a: lax.ppermute(a, "gy", [(i, i ^ 1) for i in range(8)])
    along_z = lambda a, d: lax.ppermute(a, "gz", [(i, (i + d) % 8) for i in range(8)])

    unit = jax.ShapeDtypeStruct((ROWS, HD), BF16)
    anywhere = pl.BlockSpec(memory_space=pl.ANY)
    rows_here = pltpu.VMEM(key_rows.shape, BF16)
    keep, send = pl.pallas_call(
        states_kernel,
        out_shape=(unit, unit),
        in_specs=[anywhere, anywhere],
        scratch_shapes=[rows_here, rows_here, pltpu.SemaphoreType.DMA((2, 2))],
        compiler_params=pltpu.CompilerParams(vmem_limit_bytes=8 << 20),
        cost_estimate=pl.CostEstimate(flops=10**9, bytes_accessed=10**6, transcendentals=0),
        name="states",
    )(key_rows, values)
    keys = {(0, 0): keep}
    for d in (2, 1, 3):
        keys[d, 0] = by_role(keep, d, "yx")
        keys[d, 1] = by_role(send, d, "xy", cross=True)
    keys[0, 1] = to_mate(send)

    both_lists = jnp.stack([tile_list, to_mate(tile_list)])
    lists = [both_lists] + [by_role(both_lists, d, "xy") for d in (1, 2, 3)]
    listed = lax.dynamic_slice_in_dim(jnp.stack(lists), 2 * core, 2, 3)
    listed = jnp.moveaxis(listed, 3, 0).reshape(32, 8)
    listed = jnp.repeat(listed, 16, axis=1).astype(F32)
    k = lax.iota(jnp.int32, HD) % 16
    back, other, b = k // 4, k // 2 % 2, k % 2
    key_core = jnp.where(other == 1, 1 - core, core)
    key_x = jnp.where(core == 1, (gx - back) % 4, gx)
    key_y = jnp.where(core == 0, (y - back) % 4, y)
    key_blocks = (2 * (key_x * 8 + key_y * 2 + key_core) + b).astype(F32).reshape(1, HD)

    order = [(d, c) for d in range(4) for c in range(2)]
    parts = call(partial_kernel, (unit,) * 8, 10**9, 16, "partial")(
        key_blocks, listed, *(keys[i] for i in order)
    )
    parts = dict(zip(order, parts))
    for d in (2, 1, 3):
        parts[d, 0] = by_role(parts[d, 0], -d, "xy")
        parts[d, 1] = by_role(parts[d, 1], -d, "xy", cross=True)
    parts[0, 1] = to_mate(parts[0, 1])

    qf = features(queries)
    half = out_weight.shape[1] // 2
    piece = jax.ShapeDtypeStruct((64, half), BF16)
    heads = jax.ShapeDtypeStruct((8 * HD, HD), BF16)
    right1, left0, states, sums, _ = call(
        far_kernel,
        (piece, piece, heads, heads, jax.ShapeDtypeStruct((64, queries.shape[1]), BF16)),
        10**9,
        16,
        "far",
    )(qf, out_weight, *(parts[d, c] for c in range(2) for d in range(4)))
    right1, left0 = along_z(right1, 1), along_z(left0, -1)
    term = jax.ShapeDtypeStruct((128, half), F32)
    right0, left1, f3, e2, f2, e1, f1, own, _ = call(
        project_kernel,
        (piece, piece)
        + (term,) * 5
        + (jax.ShapeDtypeStruct((64, 2 * half), F32), jax.ShapeDtypeStruct(queries.shape, BF16)),
        4 * 10**9,
        20,
        "project",
    )(qf, out_weight, states, sums)
    right0, left1 = along_z(right0, 1), along_z(left1, -1)

    def hop(term, from_left, from_right, name):
        right, left = call(hop_kernel, (piece, piece), 10**8, 4, name)(term, from_left, from_right)
        return along_z(right, 1), along_z(left, -1)

    right1, left0 = hop(f3, right1, left0, "hop3b")
    right0, left1 = hop(e2, right0, left1, "hop2a")
    right1, left0 = hop(f2, right1, left0, "hop2b")
    right0, left1 = hop(e1, right0, left1, "hop1a")
    right1, left0 = hop(f1, right1, left0, "hop1b")
    return call(last_kernel, jax.ShapeDtypeStruct((64, 2 * half), BF16), 10**8, 8, "last")(
        own, right0, left1, right1, left0
    )


def solution(mesh):
    return jax.shard_map(
        per_device,
        mesh=mesh,
        in_specs=(
            P(("gx", "gy"), "gz"),
            P(("gx", "gy"), "gz"),
            P(("gx", "gy"), "gz"),
            P(("gx", "gy"), "gz", None),
            P("gz", None),
        ),
        out_specs=P(("gx", "gy", "gz"), None),
        check_vma=False,
    )
```

```python
import jax
import jax.numpy as jnp
from jax import lax
from jax.experimental import pallas as pl
from jax.experimental.pallas import tpu as pltpu
from jax.sharding import PartitionSpec as P

BLOCK = 256
HD = 128
UNIT = 144
ROWS = 4 * UNIT
F32 = jnp.float32
BF16 = jnp.bfloat16


def call(kernel, out_shape, flops, vmem_mib, name):
    return pl.pallas_call(
        kernel,
        out_shape=out_shape,
        compiler_params=pltpu.CompilerParams(vmem_limit_bytes=vmem_mib << 20),
        cost_estimate=pl.CostEstimate(flops=flops, bytes_accessed=flops // 256, transcendentals=0),
        name=name,
    )


def features(source):
    widened = source.astype(F32)
    return jnp.where(widened > 0, widened + 1.0, jnp.exp(jnp.minimum(widened, 0.0))).astype(BF16)


def high_and_low(total):
    high = total.astype(BF16).astype(F32)
    row = lax.broadcasted_iota(jnp.int32, (16, HD), 0)
    return jnp.where(row == 0, high, jnp.where(row == 1, total - high, 0.0)).astype(BF16)


def head_columns(h):
    return pl.ds(pl.multiple_of(h * HD, HD), HD)


def chunk_rows(j):
    return pl.ds(pl.multiple_of(j * 64, 64), 64)


def states_kernel(kf_ref, v_ref, own_ref, mate_ref, keep_ref, send_ref, lists_ref):
    core = lax.rem(lax.axis_index("gy"), 2)
    ones = jnp.ones((16, BLOCK), BF16)
    entry = lax.broadcasted_iota(jnp.int32, (8, HD), 0)
    lane = lax.broadcasted_iota(jnp.int32, (8, HD), 1)
    repeat = jnp.where(lane // 16 == entry, 1.0, 0.0).astype(BF16)
    for i, list_ref in enumerate((own_ref, mate_ref)):
        for b in range(2):
            listed = list_ref[b].astype(F32).astype(BF16)
            at = i * 8 + b * 4
            lists_ref[at : at + 4, :] = jnp.dot(listed, repeat, preferred_element_type=F32)
    row = lax.broadcasted_iota(jnp.int32, (16, HD), 0)
    for u_ref, role in ((keep_ref, core), (send_ref, 1 - core)):
        for b in range(2):
            rows = pl.ds(b * BLOCK, BLOCK)
            for hh in range(2):
                at = (b * 2 + hh) * UNIT
                columns = head_columns(2 * role + hh)
                kf = kf_ref[rows, columns]
                state = lax.dot_general(
                    v_ref[rows, columns], kf, (((0,), (0,)), ((), ())), preferred_element_type=F32
                )
                u_ref[at : at + HD, :] = state.astype(BF16)
                tail = high_and_low(jnp.dot(ones, kf, preferred_element_type=F32))
                if u_ref is keep_ref:
                    other = b * 4 + 2 * (1 - core) + hh
                    tail = jnp.where(row == 2, lists_ref[pl.ds(8 + other, 1), :], tail.astype(F32))
                    tail = jnp.where(row == 3, lists_ref[pl.ds(other, 1), :], tail).astype(BF16)
                u_ref[at + HD : at + UNIT, :] = tail


def key_blocks():
    gx, gy = lax.axis_index("gx"), lax.axis_index("gy")
    y, core = gy // 2, lax.rem(gy, 2)
    k = lax.rem(lax.broadcasted_iota(jnp.int32, (256, HD), 1), 16)
    back, other, b = k // 4, lax.rem(k // 2, 2), lax.rem(k, 2)
    key_x = lax.rem(gx - back * core + 4, 4)
    key_y = lax.rem(y - back * (1 - core) + 4, 4)
    key_core = core + other * (1 - 2 * core)
    return (2 * (key_x * 8 + key_y * 2 + key_core) + b).astype(F32)


def partial_kernel(*refs):
    lists, keys, outs = refs[:4], refs[4:12], refs[12:]
    core, kb = lax.rem(lax.axis_index("gy"), 2), key_blocks()
    lane = lax.broadcasted_iota(jnp.int32, (HD, 256), 0)
    col = lax.broadcasted_iota(jnp.int32, (HD, 256), 1)
    spread = jnp.where(lax.rem(lane, 16) == col // 16, 1.0, 0.0).astype(BF16)
    row = lax.broadcasted_iota(jnp.int32, (256, 256), 0)
    col = lax.broadcasted_iota(jnp.int32, (256, 256), 1)
    same = jnp.where(lax.rem(row, 16) == lax.rem(col, 16), 1.0, 0.0)
    blocks = [(d * 2 + c, b * 2 * UNIT) for d in range(4) for c in range(2) for b in range(2)]
    for hh in range(2):
        listed = []
        for d in range(4):
            for c in range(2):
                for b in range(2):
                    if d == 0:
                        one = lists[0][pl.ds(c * 8 + b * 4 + 2 * core + hh, 1), :]
                    else:
                        at = (b * 2 + hh) * UNIT + HD
                        one = lists[d][at : at + 16, :].astype(F32)[2 + c : 3 + c, :]
                    listed.append(jnp.broadcast_to(one, (16, HD)))
        hit = jnp.where(jnp.concatenate(listed, axis=0) == kb, 1.0, 0.0).astype(BF16)
        mix = (jnp.dot(hit, spread, preferred_element_type=F32) * same).astype(BF16)
        for g in range(9):
            shift = hh * UNIT + g * 16
            pieces = [keys[d][at + shift : at + shift + 16, :] for d, at in blocks]
            summed = jnp.dot(mix, jnp.concatenate(pieces, axis=0), preferred_element_type=F32)
            for q, (d, at) in enumerate(blocks):
                piece = summed[q * 16 : q * 16 + 16, :]
                if g == 8:
                    outs[d][at + shift : at + shift + 16, :] = high_and_low(piece[0:1] + piece[1:2])
                else:
                    outs[d][at + shift : at + shift + 16, :] = piece.astype(BF16)


def attend(q_ref, state_ref, sums_ref, at, rows, columns):
    dims = (((1,), (1,)), ((), ()))
    q = q_ref[rows, columns]
    num = lax.dot_general(q, state_ref[at, :], dims, preferred_element_type=F32)
    sums = sums_ref[at, :]
    return (num / lax.dot_general(q, sums, dims, preferred_element_type=F32)).astype(BF16)


def far_kernel(qf_ref, w_ref, *refs):
    parts, (right_ref, left_ref, state_ref, sums_ref, att_ref) = (refs[:4], refs[4:8]), refs[8:]
    core, far = lax.rem(lax.axis_index("gy"), 2), lax.rem(lax.axis_index("gz") + 4, 8)
    for side in range(2):
        role = core if side == 0 else 1 - core
        for u in range(4):
            at = u * UNIT
            total = sum(p[at : at + UNIT, :].astype(F32) for p in parts[side])
            to = pl.ds(pl.multiple_of((u // 2 * 4 + 2 * role + u % 2) * HD, HD), HD)
            state_ref[to, :] = total[:HD].astype(BF16)
            key_sum = total[HD : HD + 1] + total[HD + 1 : HD + 2]
            sums_ref[to, :] = jnp.broadcast_to(key_sum, (HD, HD)).astype(BF16)
    for h in range(4):
        at = pl.ds(pl.multiple_of((far // 4 * 4 + h) * HD, HD), HD)
        columns = slice(h * HD, (h + 1) * HD)
        att_ref[:, columns] = attend(qf_ref, state_ref, sums_ref, at, chunk_rows(far), columns)
    half = w_ref.shape[1] // 2
    right_ref[...] = jnp.dot(att_ref[...], w_ref[:, half:], preferred_element_type=F32).astype(BF16)
    left_ref[...] = jnp.dot(att_ref[...], w_ref[:, :half], preferred_element_type=F32).astype(BF16)


def project_kernel(qf_ref, w_ref, state_ref, sums_ref, *refs):
    r3_ref, l3_ref, f3_ref, e2_ref, f2_ref, e1_ref, f1_ref, own_ref, att_ref = refs
    gz = lax.axis_index("gz")
    for b in range(2):
        for h in range(4):
            at, columns = pl.ds((b * 4 + h) * HD, HD), slice(h * HD, (h + 1) * HD)
            rows = pl.ds(b * BLOCK, BLOCK)
            att_ref[rows, columns] = attend(qf_ref, state_ref, sums_ref, at, rows, columns)
    hops = (3, 5, 2, 6, 1, 7, 0)
    lhs = jnp.concatenate([att_ref[chunk_rows(lax.rem(gz + hop, 8)), :] for hop in hops], axis=0)
    half = w_ref.shape[1] // 2
    for i in range(2):
        for c in range(0, half, 512):
            out = jnp.dot(lhs, w_ref[:, i * half + c : i * half + c + 512], preferred_element_type=F32)
            cols = slice(c, c + 512)
            for n, (e_ref, f_ref) in enumerate(((None, f3_ref), (e2_ref, f2_ref), (e1_ref, f1_ref))):
                right, left = out[n * 128 : n * 128 + 64], out[n * 128 + 64 : n * 128 + 128]
                early = (right, left)[i]
                f_ref[(64, 0)[i] : (128, 64)[i], cols] = (left, right)[i]
                if e_ref is None:
                    (r3_ref, l3_ref)[i][:, cols] = early.astype(BF16)
                else:
                    e_ref[(0, 64)[i] : (64, 128)[i], cols] = early
            own_ref[:, i * half + c : i * half + c + 512] = out[384:448]


def hop_kernel(term_ref, from_left_ref, from_right_ref, right_ref, left_ref):
    right_ref[...] = (term_ref[:64, :] + from_left_ref[...].astype(F32)).astype(BF16)
    left_ref[...] = (term_ref[64:, :] + from_right_ref[...].astype(F32)).astype(BF16)


def last_kernel(own_ref, right0, left1, right1, left0, out_ref):
    half = own_ref.shape[1] // 2
    for i, (a, b) in enumerate(((right0, left0), (right1, left1))):
        out_ref[:, i * half : (i + 1) * half] = (
            own_ref[:, i * half : (i + 1) * half] + a[...].astype(F32) + b[...].astype(F32)
        ).astype(BF16)


def per_device(queries, key_rows, values, tile_list, out_weight):
    def by_role(a, d, axes, cross=False):
        pairs = []
        for i in range(4):
            for j in range(4):
                for c in range(2):
                    to = ((i + d) % 4, j) if axes[c] == "x" else (i, (j + d) % 4)
                    pairs.append((i * 8 + j * 2 + c, to[0] * 8 + to[1] * 2 + (c ^ cross)))
        return lax.ppermute(a, ("gx", "gy"), pairs)

    to_mate = lambda a: lax.ppermute(a, "gy", [(i, i ^ 1) for i in range(8)])
    along_z = lambda a, d: lax.ppermute(a, "gz", [(i, (i + d) % 8) for i in range(8)])

    unit = jax.ShapeDtypeStruct((ROWS, HD), BF16)
    keep, send, lists = call(
        states_kernel, (unit, unit, jax.ShapeDtypeStruct((16, HD), F32)), 10**9, 8, "states"
    )(features(key_rows), values, tile_list, to_mate(tile_list))
    keys = {(0, 0): keep}
    for d in (2, 1, 3):
        keys[d, 0] = by_role(keep, d, "yx")
        keys[d, 1] = by_role(send, d, "xy", cross=True)
    keys[0, 1] = to_mate(send)

    lists = [lists] + [to_mate(keys[d, 0]) for d in (1, 2, 3)]
    order = [(d, c) for d in range(4) for c in range(2)]
    parts = call(partial_kernel, (unit,) * 8, 10**9, 16, "partial")(
        *lists, *(keys[i] for i in order)
    )
    parts = dict(zip(order, parts))
    for d in (2, 1, 3):
        parts[d, 0] = by_role(parts[d, 0], -d, "xy")
        parts[d, 1] = by_role(parts[d, 1], -d, "xy", cross=True)
    parts[0, 1] = to_mate(parts[0, 1])

    qf = features(queries)
    half = out_weight.shape[1] // 2
    piece = jax.ShapeDtypeStruct((64, half), BF16)
    heads = jax.ShapeDtypeStruct((8 * HD, HD), BF16)
    right1, left0, states, sums, _ = call(
        far_kernel,
        (piece, piece, heads, heads, jax.ShapeDtypeStruct((64, queries.shape[1]), BF16)),
        10**9,
        16,
        "far",
    )(qf, out_weight, *(parts[d, c] for c in range(2) for d in range(4)))
    right1, left0 = along_z(right1, 1), along_z(left0, -1)
    term = jax.ShapeDtypeStruct((128, half), F32)
    right0, left1, f3, e2, f2, e1, f1, own, _ = call(
        project_kernel,
        (piece, piece)
        + (term,) * 5
        + (jax.ShapeDtypeStruct((64, 2 * half), F32), jax.ShapeDtypeStruct(queries.shape, BF16)),
        4 * 10**9,
        20,
        "project",
    )(qf, out_weight, states, sums)
    right0, left1 = along_z(right0, 1), along_z(left1, -1)

    def hop(term, from_left, from_right, name):
        right, left = call(hop_kernel, (piece, piece), 10**8, 4, name)(term, from_left, from_right)
        return along_z(right, 1), along_z(left, -1)

    right1, left0 = hop(f3, right1, left0, "hop3b")
    right0, left1 = hop(e2, right0, left1, "hop2a")
    right1, left0 = hop(f2, right1, left0, "hop2b")
    right0, left1 = hop(e1, right0, left1, "hop1a")
    right1, left0 = hop(f1, right1, left0, "hop1b")
    return call(last_kernel, jax.ShapeDtypeStruct((64, 2 * half), BF16), 10**8, 8, "last")(
        own, right0, left1, right1, left0
    )


def solution(mesh):
    return jax.shard_map(
        per_device,
        mesh=mesh,
        in_specs=(
            P(("gx", "gy"), "gz"),
            P(("gx", "gy"), "gz"),
            P(("gx", "gy"), "gz"),
            P(("gx", "gy"), "gz", None),
            P("gz", None),
        ),
        out_specs=P(("gx", "gy", "gz"), None),
        check_vma=False,
    )
```

```python
import jax
import jax.numpy as jnp
from jax import lax
from jax.experimental import pallas as pl
from jax.experimental.pallas import tpu as pltpu
from jax.sharding import PartitionSpec as P

BLOCK = 256
HD = 128
UNIT = 144
ROWS = 4 * UNIT
F32 = jnp.float32
BF16 = jnp.bfloat16


def call(kernel, out_shape, flops, vmem_mib):
    return pl.pallas_call(
        kernel,
        out_shape=out_shape,
        compiler_params=pltpu.CompilerParams(vmem_limit_bytes=vmem_mib << 20),
        cost_estimate=pl.CostEstimate(flops=flops, bytes_accessed=flops // 256, transcendentals=0),
    )


def features(source):
    widened = source.astype(F32)
    return jnp.where(widened > 0, widened + 1.0, jnp.exp(jnp.minimum(widened, 0.0))).astype(BF16)


def high_and_low(total):
    high = total.astype(BF16).astype(F32)
    row = lax.broadcasted_iota(jnp.int32, (16, HD), 0)
    return jnp.where(row == 0, high, jnp.where(row == 1, total - high, 0.0)).astype(BF16)


def head_columns(h):
    return pl.ds(pl.multiple_of(h * HD, HD), HD)


def chunk_rows(j):
    return pl.ds(pl.multiple_of(j * 64, 64), 64)


def states_kernel(kv_ref, own_ref, mate_ref, keep_ref, send_ref, lists_ref):
    core = lax.rem(lax.axis_index("gy"), 2)
    ones = jnp.ones((16, BLOCK), BF16)
    entry = lax.broadcasted_iota(jnp.int32, (8, HD), 0)
    lane = lax.broadcasted_iota(jnp.int32, (8, HD), 1)
    repeat = jnp.where(lane // 16 == entry, 1.0, 0.0).astype(BF16)
    for i, list_ref in enumerate((own_ref, mate_ref)):
        for b in range(2):
            listed = list_ref[b].astype(F32).astype(BF16)
            at = i * 8 + b * 4
            lists_ref[at : at + 4, :] = jnp.dot(listed, repeat, preferred_element_type=F32)
    row = lax.broadcasted_iota(jnp.int32, (16, HD), 0)
    for u_ref, role in ((keep_ref, core), (send_ref, 1 - core)):
        for b in range(2):
            rows = pl.ds(b * BLOCK, BLOCK)
            for hh in range(2):
                at = (b * 2 + hh) * UNIT
                columns = head_columns(2 * role + hh)
                kf = kv_ref[rows, columns]
                state = lax.dot_general(
                    kv_ref[pl.ds((2 + b) * BLOCK, BLOCK), columns], kf, (((0,), (0,)), ((), ())), preferred_element_type=F32
                )
                u_ref[at : at + HD, :] = state.astype(BF16)
                tail = high_and_low(jnp.dot(ones, kf, preferred_element_type=F32))
                if u_ref is keep_ref:
                    other = b * 4 + 2 * (1 - core) + hh
                    tail = jnp.where(row == 2, lists_ref[pl.ds(8 + other, 1), :], tail.astype(F32))
                    tail = jnp.where(row == 3, lists_ref[pl.ds(other, 1), :], tail).astype(BF16)
                u_ref[at + HD : at + UNIT, :] = tail


def key_blocks():
    gx, gy = lax.axis_index("gx"), lax.axis_index("gy")
    y, core = gy // 2, lax.rem(gy, 2)
    k = lax.rem(lax.broadcasted_iota(jnp.int32, (256, HD), 1), 16)
    back, other, b = k // 4, lax.rem(k // 2, 2), lax.rem(k, 2)
    key_x = lax.rem(gx - back * core + 4, 4)
    key_y = lax.rem(y - back * (1 - core) + 4, 4)
    key_core = core + other * (1 - 2 * core)
    return (2 * (key_x * 8 + key_y * 2 + key_core) + b).astype(F32)


def partial_kernel(*refs):
    lists, keys, outs = refs[:4], refs[4:12], refs[12:]
    core, kb = lax.rem(lax.axis_index("gy"), 2), key_blocks()
    lane = lax.broadcasted_iota(jnp.int32, (HD, 256), 0)
    col = lax.broadcasted_iota(jnp.int32, (HD, 256), 1)
    spread = jnp.where(lax.rem(lane, 16) == col // 16, 1.0, 0.0).astype(BF16)
    row = lax.broadcasted_iota(jnp.int32, (256, 256), 0)
    col = lax.broadcasted_iota(jnp.int32, (256, 256), 1)
    same = jnp.where(lax.rem(row, 16) == lax.rem(col, 16), 1.0, 0.0)
    blocks = [(d * 2 + c, b * 2 * UNIT) for d in range(4) for c in range(2) for b in range(2)]
    for hh in range(2):
        listed = []
        for d in range(4):
            for c in range(2):
                for b in range(2):
                    if d == 0:
                        one = lists[0][pl.ds(c * 8 + b * 4 + 2 * core + hh, 1), :]
                    else:
                        at = (b * 2 + hh) * UNIT + HD
                        one = lists[d][at : at + 16, :].astype(F32)[2 + c : 3 + c, :]
                    listed.append(jnp.broadcast_to(one, (16, HD)))
        hit = jnp.where(jnp.concatenate(listed, axis=0) == kb, 1.0, 0.0).astype(BF16)
        mix = (jnp.dot(hit, spread, preferred_element_type=F32) * same).astype(BF16)
        for g in range(9):
            shift = hh * UNIT + g * 16
            pieces = [keys[d][at + shift : at + shift + 16, :] for d, at in blocks]
            summed = jnp.dot(mix, jnp.concatenate(pieces, axis=0), preferred_element_type=F32)
            for q, (d, at) in enumerate(blocks):
                piece = summed[q * 16 : q * 16 + 16, :]
                if g == 8:
                    outs[d][at + shift : at + shift + 16, :] = high_and_low(piece[0:1] + piece[1:2])
                else:
                    outs[d][at + shift : at + shift + 16, :] = piece.astype(BF16)


def attend(q_ref, state_ref, sums_ref, at, rows, columns):
    dims = (((1,), (1,)), ((), ()))
    q = q_ref[rows, columns]
    num = lax.dot_general(q, state_ref[at, :], dims, preferred_element_type=F32)
    sums = sums_ref[at, :]
    return (num / lax.dot_general(q, sums, dims, preferred_element_type=F32)).astype(BF16)


def far_kernel(qf_ref, w_ref, *refs):
    parts, (right_ref, left_ref, state_ref, sums_ref, att_ref) = (refs[:4], refs[4:8]), refs[8:]
    core, far = lax.rem(lax.axis_index("gy"), 2), lax.rem(lax.axis_index("gz") + 4, 8)
    for side in range(2):
        role = core if side == 0 else 1 - core
        for u in range(4):
            at = u * UNIT
            total = sum(p[at : at + UNIT, :].astype(F32) for p in parts[side])
            to = pl.ds(pl.multiple_of((u // 2 * 4 + 2 * role + u % 2) * HD, HD), HD)
            state_ref[to, :] = total[:HD].astype(BF16)
            key_sum = total[HD : HD + 1] + total[HD + 1 : HD + 2]
            sums_ref[to, :] = jnp.broadcast_to(key_sum, (HD, HD)).astype(BF16)
    for h in range(4):
        at = pl.ds(pl.multiple_of((far // 4 * 4 + h) * HD, HD), HD)
        columns = slice(h * HD, (h + 1) * HD)
        att_ref[:, columns] = attend(qf_ref, state_ref, sums_ref, at, chunk_rows(far), columns)
    half = w_ref.shape[1] // 2
    right_ref[...] = jnp.dot(att_ref[...], w_ref[:, half:], preferred_element_type=F32).astype(BF16)
    left_ref[...] = jnp.dot(att_ref[...], w_ref[:, :half], preferred_element_type=F32).astype(BF16)


def project_kernel(qf_ref, w_ref, state_ref, sums_ref, *refs):
    r3_ref, l3_ref, f3_ref, e2_ref, f2_ref, e1_ref, f1_ref, own_ref, att_ref = refs
    gz = lax.axis_index("gz")
    for b in range(2):
        for h in range(4):
            at, columns = pl.ds((b * 4 + h) * HD, HD), slice(h * HD, (h + 1) * HD)
            rows = pl.ds(b * BLOCK, BLOCK)
            att_ref[rows, columns] = attend(qf_ref, state_ref, sums_ref, at, rows, columns)
    hops = (3, 5, 2, 6, 1, 7, 0)
    lhs = jnp.concatenate([att_ref[chunk_rows(lax.rem(gz + hop, 8)), :] for hop in hops], axis=0)
    half = w_ref.shape[1] // 2
    for i in range(2):
        for c in range(0, half, 512):
            out = jnp.dot(lhs, w_ref[:, i * half + c : i * half + c + 512], preferred_element_type=F32)
            cols = slice(c, c + 512)
            for n, (e_ref, f_ref) in enumerate(((None, f3_ref), (e2_ref, f2_ref), (e1_ref, f1_ref))):
                right, left = out[n * 128 : n * 128 + 64], out[n * 128 + 64 : n * 128 + 128]
                early = (right, left)[i]
                f_ref[(64, 0)[i] : (128, 64)[i], cols] = (left, right)[i]
                if e_ref is None:
                    (r3_ref, l3_ref)[i][:, cols] = early.astype(BF16)
                else:
                    e_ref[(0, 64)[i] : (64, 128)[i], cols] = early
            own_ref[:, i * half + c : i * half + c + 512] = out[384:448]


def hop_kernel(term_ref, from_left_ref, from_right_ref, right_ref, left_ref):
    right_ref[...] = (term_ref[:64, :] + from_left_ref[...].astype(F32)).astype(BF16)
    left_ref[...] = (term_ref[64:, :] + from_right_ref[...].astype(F32)).astype(BF16)


def last_kernel(own_ref, right0, left1, right1, left0, out_ref):
    half = own_ref.shape[1] // 2
    for i, (a, b) in enumerate(((right0, left0), (right1, left1))):
        out_ref[:, i * half : (i + 1) * half] = (
            own_ref[:, i * half : (i + 1) * half] + a[...].astype(F32) + b[...].astype(F32)
        ).astype(BF16)


def per_device(queries, key_rows, values, tile_list, out_weight):
    def by_role(a, d, axes, cross=False):
        pairs = []
        for i in range(4):
            for j in range(4):
                for c in range(2):
                    to = ((i + d) % 4, j) if axes[c] == "x" else (i, (j + d) % 4)
                    pairs.append((i * 8 + j * 2 + c, to[0] * 8 + to[1] * 2 + (c ^ cross)))
        return lax.ppermute(a, ("gx", "gy"), pairs)

    to_mate = lambda a: lax.ppermute(a, "gy", [(i, i ^ 1) for i in range(8)])
    along_z = lambda a, d: lax.ppermute(a, "gz", [(i, (i + d) % 8) for i in range(8)])

    unit = jax.ShapeDtypeStruct((ROWS, HD), BF16)
    kv = jnp.concatenate([features(key_rows), values])
    keep, send, lists = call(
        states_kernel, (unit, unit, jax.ShapeDtypeStruct((16, HD), F32)), 10**9, 8
    )(kv, tile_list, to_mate(tile_list))
    keys = {(0, 0): keep}
    for d in (2, 1, 3):
        keys[d, 0] = by_role(keep, d, "yx")
        keys[d, 1] = by_role(send, d, "xy", cross=True)
    keys[0, 1] = to_mate(send)

    lists = [lists] + [to_mate(keys[d, 0]) for d in (1, 2, 3)]
    order = [(d, c) for d in range(4) for c in range(2)]
    parts = call(partial_kernel, (unit,) * 8, 10**9, 16)(*lists, *(keys[i] for i in order))
    parts = dict(zip(order, parts))
    for d in (2, 1, 3):
        parts[d, 0] = by_role(parts[d, 0], -d, "xy")
        parts[d, 1] = by_role(parts[d, 1], -d, "xy", cross=True)
    parts[0, 1] = to_mate(parts[0, 1])

    qf = features(queries)
    half = out_weight.shape[1] // 2
    piece = jax.ShapeDtypeStruct((64, half), BF16)
    heads = jax.ShapeDtypeStruct((8 * HD, HD), BF16)
    right1, left0, states, sums, _ = call(
        far_kernel,
        (piece, piece, heads, heads, jax.ShapeDtypeStruct((64, queries.shape[1]), BF16)),
        10**9,
        16,
    )(qf, out_weight, *(parts[d, c] for c in range(2) for d in range(4)))
    right1, left0 = along_z(right1, 1), along_z(left0, -1)
    term = jax.ShapeDtypeStruct((128, half), F32)
    right0, left1, f3, e2, f2, e1, f1, own, _ = call(
        project_kernel,
        (piece, piece)
        + (term,) * 5
        + (jax.ShapeDtypeStruct((64, 2 * half), F32), jax.ShapeDtypeStruct(queries.shape, BF16)),
        4 * 10**9,
        20,
    )(qf, out_weight, states, sums)
    right0, left1 = along_z(right0, 1), along_z(left1, -1)

    def hop(term, from_left, from_right):
        right, left = call(hop_kernel, (piece, piece), 10**8, 4)(term, from_left, from_right)
        return along_z(right, 1), along_z(left, -1)

    right1, left0 = hop(f3, right1, left0)
    right0, left1 = hop(e2, right0, left1)
    right1, left0 = hop(f2, right1, left0)
    right0, left1 = hop(e1, right0, left1)
    right1, left0 = hop(f1, right1, left0)
    return call(last_kernel, jax.ShapeDtypeStruct((64, 2 * half), BF16), 10**8, 8)(
        own, right0, left1, right1, left0
    )


def solution(mesh):
    return jax.shard_map(
        per_device,
        mesh=mesh,
        in_specs=(
            P(("gx", "gy"), "gz"),
            P(("gx", "gy"), "gz"),
            P(("gx", "gy"), "gz"),
            P(("gx", "gy"), "gz", None),
            P("gz", None),
        ),
        out_specs=P(("gx", "gy", "gz"), None),
        check_vma=False,
    )
```

```python
import jax
import jax.numpy as jnp
from jax import lax
from jax.experimental import pallas as pl
from jax.experimental.pallas import tpu as pltpu
from jax.sharding import PartitionSpec as P

BLOCK = 256
HD = 128
STATES = 4 * HD
ROWS = STATES + 16
F32 = jnp.float32
BF16 = jnp.bfloat16


def call(kernel, out_shape, flops, vmem_mib):
    return pl.pallas_call(
        kernel,
        out_shape=out_shape,
        compiler_params=pltpu.CompilerParams(vmem_limit_bytes=vmem_mib << 20),
        cost_estimate=pl.CostEstimate(flops=flops, bytes_accessed=flops // 256, transcendentals=0),
    )


def features(source):
    widened = source.astype(F32)
    return jnp.where(widened > 0, widened + 1.0, jnp.exp(jnp.minimum(widened, 0.0))).astype(BF16)


def high_and_low(total):
    high = total.astype(BF16).astype(F32)
    return high, total - high


def with_rows(tail, at, rows):
    row = lax.broadcasted_iota(jnp.int32, (16, HD), 0)
    for i, one in enumerate(rows):
        tail = jnp.where(row == at + i, one, tail)
    return tail


def head_columns(h):
    return pl.ds(pl.multiple_of(h * HD, HD), HD)


def chunk_rows(j):
    return pl.ds(pl.multiple_of(j * 64, 64), 64)


def states_kernel(kv_ref, own_ref, mate_ref, keep_ref, send_ref, lists_ref):
    core = lax.rem(lax.axis_index("gy"), 2)
    ones = jnp.ones((16, BLOCK), BF16)
    entry = lax.broadcasted_iota(jnp.int32, (8, HD), 0)
    lane = lax.broadcasted_iota(jnp.int32, (8, HD), 1)
    repeat = jnp.where(lane // 16 == entry, 1.0, 0.0).astype(BF16)
    for i, list_ref in enumerate((own_ref, mate_ref)):
        for b in range(2):
            listed = list_ref[b].astype(F32).astype(BF16)
            at = i * 8 + b * 4
            lists_ref[at : at + 4, :] = jnp.dot(listed, repeat, preferred_element_type=F32)
    for u_ref, role in ((keep_ref, core), (send_ref, 1 - core)):
        tail = jnp.zeros((16, HD), F32)
        for b in range(2):
            rows = pl.ds(b * BLOCK, BLOCK)
            for hh in range(2):
                u = b * 2 + hh
                columns = head_columns(2 * role + hh)
                kf = kv_ref[rows, columns]
                state = lax.dot_general(
                    kv_ref[pl.ds((2 + b) * BLOCK, BLOCK), columns],
                    kf,
                    (((0,), (0,)), ((), ())),
                    preferred_element_type=F32,
                )
                u_ref[u * HD : (u + 1) * HD, :] = state.astype(BF16)
                total = jnp.dot(ones, kf, preferred_element_type=F32)[:1]
                tail = with_rows(tail, 2 * u, high_and_low(total))
                if u_ref is keep_ref:
                    other = b * 4 + 2 * (1 - core) + hh
                    both = [lists_ref[pl.ds(8 * i + other, 1), :] for i in (1, 0)]
                    tail = with_rows(tail, 8 + 2 * u, both)
        u_ref[STATES:, :] = tail.astype(BF16)


def key_blocks():
    gx, gy = lax.axis_index("gx"), lax.axis_index("gy")
    y, core = gy // 2, lax.rem(gy, 2)
    k = lax.rem(lax.broadcasted_iota(jnp.int32, (256, HD), 1), 16)
    back, other, b = k // 4, lax.rem(k // 2, 2), lax.rem(k, 2)
    key_x = lax.rem(gx - back * core + 4, 4)
    key_y = lax.rem(y - back * (1 - core) + 4, 4)
    key_core = core + other * (1 - 2 * core)
    return (2 * (key_x * 8 + key_y * 2 + key_core) + b).astype(F32)


def partial_kernel(*refs):
    lists, keys, outs = refs[:4], refs[4:12], refs[12:]
    core, kb = lax.rem(lax.axis_index("gy"), 2), key_blocks()
    lane = lax.broadcasted_iota(jnp.int32, (HD, 256), 0)
    col = lax.broadcasted_iota(jnp.int32, (HD, 256), 1)
    spread = jnp.where(lax.rem(lane, 16) == col // 16, 1.0, 0.0).astype(BF16)
    row = lax.broadcasted_iota(jnp.int32, (256, 256), 0)
    col = lax.broadcasted_iota(jnp.int32, (256, 256), 1)
    same = jnp.where(lax.rem(row, 16) == lax.rem(col, 16), 1.0, 0.0)
    blocks = [(d * 2 + c, b) for d in range(4) for c in range(2) for b in range(2)]
    tile_row = lax.broadcasted_iota(jnp.int32, (16, HD), 0)
    tails = [ref[STATES:, :].astype(F32) for ref in keys]
    out_tails = [jnp.zeros((16, HD), F32)] * 8
    for hh in range(2):
        listed = []
        for i, b in blocks:
            if i < 2:
                one = lists[0][pl.ds(i * 8 + b * 4 + 2 * core + hh, 1), :]
            else:
                at = 8 + 2 * (b * 2 + hh) + i % 2
                one = lists[i // 2][STATES:, :].astype(F32)[at : at + 1, :]
            listed.append(jnp.broadcast_to(one, (16, HD)))
        hit = jnp.where(jnp.concatenate(listed, axis=0) == kb, 1.0, 0.0).astype(BF16)
        mix = (jnp.dot(hit, spread, preferred_element_type=F32) * same).astype(BF16)
        for g in range(8):
            shift = hh * HD + g * 16
            pieces = [keys[i][b * 2 * HD + shift : b * 2 * HD + shift + 16, :] for i, b in blocks]
            summed = jnp.dot(mix, jnp.concatenate(pieces, axis=0), preferred_element_type=F32)
            for q, (i, b) in enumerate(blocks):
                at = b * 2 * HD + shift
                outs[i][at : at + 16, :] = summed[q * 16 : q * 16 + 16, :].astype(BF16)
        pieces = [
            jnp.where(tile_row // 2 == b * 2 + hh, tails[i], 0.0).astype(BF16) for i, b in blocks
        ]
        summed = jnp.dot(mix, jnp.concatenate(pieces, axis=0), preferred_element_type=F32)
        for q, (i, b) in enumerate(blocks):
            total = jnp.sum(summed[q * 16 : q * 16 + 8, :], axis=0, keepdims=True)
            out_tails[i] = with_rows(out_tails[i], 2 * (b * 2 + hh), high_and_low(total))
    for out_ref, tail in zip(outs, out_tails):
        out_ref[STATES:, :] = tail.astype(BF16)


def attend(q_ref, state_ref, sums_ref, at, rows, columns):
    dims = (((1,), (1,)), ((), ()))
    q = q_ref[rows, columns]
    num = lax.dot_general(q, state_ref[at, :], dims, preferred_element_type=F32)
    sums = sums_ref[at, :]
    return (num / lax.dot_general(q, sums, dims, preferred_element_type=F32)).astype(BF16)


def far_kernel(qf_ref, w_ref, *refs):
    parts, (right_ref, left_ref, state_ref, sums_ref, att_ref) = (refs[:4], refs[4:8]), refs[8:]
    core, far = lax.rem(lax.axis_index("gy"), 2), lax.rem(lax.axis_index("gz") + 4, 8)
    for side in range(2):
        role = core if side == 0 else 1 - core
        tail = sum(p[STATES:, :].astype(F32) for p in parts[side])
        for u in range(4):
            total = sum(p[u * HD : (u + 1) * HD, :].astype(F32) for p in parts[side])
            to = pl.ds(pl.multiple_of((u // 2 * 4 + 2 * role + u % 2) * HD, HD), HD)
            state_ref[to, :] = total.astype(BF16)
            key_sum = tail[2 * u : 2 * u + 1] + tail[2 * u + 1 : 2 * u + 2]
            sums_ref[to, :] = jnp.broadcast_to(key_sum, (HD, HD)).astype(BF16)
    for h in range(4):
        at = pl.ds(pl.multiple_of((far // 4 * 4 + h) * HD, HD), HD)
        columns = slice(h * HD, (h + 1) * HD)
        att_ref[:, columns] = attend(qf_ref, state_ref, sums_ref, at, chunk_rows(far), columns)
    half = w_ref.shape[1] // 2
    right_ref[...] = jnp.dot(att_ref[...], w_ref[:, half:], preferred_element_type=F32).astype(BF16)
    left_ref[...] = jnp.dot(att_ref[...], w_ref[:, :half], preferred_element_type=F32).astype(BF16)


def project_kernel(qf_ref, w_ref, state_ref, sums_ref, *refs):
    r3_ref, l3_ref, f3_ref, e2_ref, f2_ref, e1_ref, f1_ref, own_ref, att_ref = refs
    gz = lax.axis_index("gz")
    for b in range(2):
        for h in range(4):
            at, columns = pl.ds((b * 4 + h) * HD, HD), slice(h * HD, (h + 1) * HD)
            rows = pl.ds(b * BLOCK, BLOCK)
            att_ref[rows, columns] = attend(qf_ref, state_ref, sums_ref, at, rows, columns)
    hops = (3, 5, 2, 6, 1, 7, 0)
    lhs = jnp.concatenate([att_ref[chunk_rows(lax.rem(gz + hop, 8)), :] for hop in hops], axis=0)
    half = w_ref.shape[1] // 2
    for i in range(2):
        for c in range(0, half, 512):
            out = jnp.dot(lhs, w_ref[:, i * half + c : i * half + c + 512], preferred_element_type=F32)
            cols = slice(c, c + 512)
            for n, (e_ref, f_ref) in enumerate(((None, f3_ref), (e2_ref, f2_ref), (e1_ref, f1_ref))):
                right, left = out[n * 128 : n * 128 + 64], out[n * 128 + 64 : n * 128 + 128]
                early = (right, left)[i]
                f_ref[(64, 0)[i] : (128, 64)[i], cols] = (left, right)[i]
                if e_ref is None:
                    (r3_ref, l3_ref)[i][:, cols] = early.astype(BF16)
                else:
                    e_ref[(0, 64)[i] : (64, 128)[i], cols] = early
            own_ref[:, i * half + c : i * half + c + 512] = out[384:448]


def hop_kernel(term_ref, from_left_ref, from_right_ref, right_ref, left_ref):
    right_ref[...] = (term_ref[:64, :] + from_left_ref[...].astype(F32)).astype(BF16)
    left_ref[...] = (term_ref[64:, :] + from_right_ref[...].astype(F32)).astype(BF16)


def last_kernel(own_ref, right0, left1, right1, left0, out_hbm, out_ref, sems):
    half, step = own_ref.shape[1] // 2, own_ref.shape[1] // 4
    copies = []
    for i, (a, b) in enumerate(((right0, left0), (right1, left1))):
        for c in range(0, half, step):
            cols = slice(i * half + c, i * half + c + step)
            out_ref[:, cols] = (
                own_ref[:, cols] + a[:, c : c + step].astype(F32) + b[:, c : c + step].astype(F32)
            ).astype(BF16)
            to = pl.ds(i * half + c, step)
            copies.append(
                pltpu.make_async_copy(out_ref.at[:, to], out_hbm.at[:, to], sems.at[len(copies)])
            )
            copies[-1].start()
    for copy in copies:
        copy.wait()


def per_device(queries, key_rows, values, tile_list, out_weight):
    def by_role(a, d, axes, cross=False):
        pairs = []
        for i in range(4):
            for j in range(4):
                for c in range(2):
                    to = ((i + d) % 4, j) if axes[c] == "x" else (i, (j + d) % 4)
                    pairs.append((i * 8 + j * 2 + c, to[0] * 8 + to[1] * 2 + (c ^ cross)))
        return lax.ppermute(a, ("gx", "gy"), pairs)

    to_mate = lambda a: lax.ppermute(a, "gy", [(i, i ^ 1) for i in range(8)])
    along_z = lambda a, d: lax.ppermute(a, "gz", [(i, (i + d) % 8) for i in range(8)])

    unit = jax.ShapeDtypeStruct((ROWS, HD), BF16)
    kv = jnp.concatenate([features(key_rows), values])
    keep, send, lists = call(
        states_kernel, (unit, unit, jax.ShapeDtypeStruct((16, HD), F32)), 10**9, 8
    )(kv, tile_list, to_mate(tile_list))
    keys = {(0, 0): keep}
    keys[1, 0] = by_role(keep, 1, "yx")
    keys[3, 1] = by_role(send, 3, "xy", cross=True)
    keys[3, 0] = by_role(keep, 3, "yx")
    keys[1, 1] = by_role(send, 1, "xy", cross=True)
    keys[2, 0] = by_role(keys[1, 0], 1, "yx")
    keys[2, 1] = by_role(keys[3, 1], 3, "yx")
    keys[0, 1] = to_mate(send)

    lists = [lists]
    for d in (1, 2, 3):
        lists.append(to_mate(keys[d, 0]))
    order = [(d, c) for d in range(4) for c in range(2)]
    parts = call(partial_kernel, (unit,) * 8, 10**9, 16)(*lists, *(keys[i] for i in order))
    parts = dict(zip(order, parts))
    for d in (2, 1, 3):
        parts[d, 0] = by_role(parts[d, 0], -d, "xy")
        parts[d, 1] = by_role(parts[d, 1], -d, "xy", cross=True)
    parts[0, 1] = to_mate(parts[0, 1])

    qf = features(queries)
    half = out_weight.shape[1] // 2
    piece = jax.ShapeDtypeStruct((64, half), BF16)
    heads = jax.ShapeDtypeStruct((8 * HD, HD), BF16)
    right1, left0, states, sums, _ = call(
        far_kernel,
        (piece, piece, heads, heads, jax.ShapeDtypeStruct((64, queries.shape[1]), BF16)),
        10**9,
        16,
    )(qf, out_weight, *(parts[d, c] for c in range(2) for d in range(4)))
    right1, left0 = along_z(right1, 1), along_z(left0, -1)
    term = jax.ShapeDtypeStruct((128, half), F32)
    right0, left1, f3, e2, f2, e1, f1, own, _ = call(
        project_kernel,
        (piece, piece)
        + (term,) * 5
        + (jax.ShapeDtypeStruct((64, 2 * half), F32), jax.ShapeDtypeStruct(queries.shape, BF16)),
        4 * 10**9,
        20,
    )(qf, out_weight, states, sums)
    right0, left1 = along_z(right0, 1), along_z(left1, -1)

    def hop(term, from_left, from_right):
        right, left = call(hop_kernel, (piece, piece), 10**8, 4)(term, from_left, from_right)
        return along_z(right, 1), along_z(left, -1)

    right1, left0 = hop(f3, right1, left0)
    right0, left1 = hop(e2, right0, left1)
    right1, left0 = hop(f2, right1, left0)
    right0, left1 = hop(e1, right0, left1)
    right1, left0 = hop(f1, right1, left0)
    return pl.pallas_call(
        last_kernel,
        out_shape=jax.ShapeDtypeStruct((64, 2 * half), BF16),
        out_specs=pl.BlockSpec(memory_space=pltpu.HBM),
        scratch_shapes=[pltpu.VMEM((64, 2 * half), BF16), pltpu.SemaphoreType.DMA((4,))],
        compiler_params=pltpu.CompilerParams(vmem_limit_bytes=8 << 20),
        cost_estimate=pl.CostEstimate(flops=10**8, bytes_accessed=10**6, transcendentals=0),
        name="last",
    )(own, right0, left1, right1, left0)


def solution(mesh):
    return jax.shard_map(
        per_device,
        mesh=mesh,
        in_specs=(
            P(("gx", "gy"), "gz"),
            P(("gx", "gy"), "gz"),
            P(("gx", "gy"), "gz"),
            P(("gx", "gy"), "gz", None),
            P("gz", None),
        ),
        out_specs=P(("gx", "gy", "gz"), None),
        check_vma=False,
    )
```

```python
import jax
import jax.numpy as jnp
from jax import lax
from jax.experimental import pallas as pl
from jax.experimental.pallas import tpu as pltpu
from jax.sharding import PartitionSpec as P

BLOCK = 256
HD = 128
STATES = 4 * HD
ROWS = STATES + 16
F32 = jnp.float32
BF16 = jnp.bfloat16


def call(kernel, out_shape, flops, vmem_mib):
    return pl.pallas_call(
        kernel,
        out_shape=out_shape,
        compiler_params=pltpu.CompilerParams(vmem_limit_bytes=vmem_mib << 20),
        cost_estimate=pl.CostEstimate(flops=flops, bytes_accessed=flops // 256, transcendentals=0),
    )


def features(source):
    widened = source.astype(F32)
    return jnp.where(widened > 0, widened + 1.0, jnp.exp(jnp.minimum(widened, 0.0))).astype(BF16)


def high_and_low(total):
    high = total.astype(BF16).astype(F32)
    return high, total - high


def with_rows(tail, at, rows):
    row = lax.broadcasted_iota(jnp.int32, (16, HD), 0)
    for i, one in enumerate(rows):
        tail = jnp.where(row == at + i, one, tail)
    return tail


def head_columns(h):
    return pl.ds(pl.multiple_of(h * HD, HD), HD)


def chunk_rows(j):
    return pl.ds(pl.multiple_of(j * 64, 64), 64)


def states_kernel(kv_ref, own_ref, mate_ref, keep_ref, send_ref, lists_ref):
    core = lax.rem(lax.axis_index("gy"), 2)
    ones = jnp.ones((16, BLOCK), BF16)
    entry = lax.broadcasted_iota(jnp.int32, (8, HD), 0)
    lane = lax.broadcasted_iota(jnp.int32, (8, HD), 1)
    repeat = jnp.where(lane // 16 == entry, 1.0, 0.0).astype(BF16)
    for i, list_ref in enumerate((own_ref, mate_ref)):
        for b in range(2):
            listed = list_ref[b].astype(F32).astype(BF16)
            at = i * 8 + b * 4
            lists_ref[at : at + 4, :] = jnp.dot(listed, repeat, preferred_element_type=F32)
    for u_ref, role in ((keep_ref, core), (send_ref, 1 - core)):
        tail = jnp.zeros((16, HD), F32)
        for b in range(2):
            rows = pl.ds(b * BLOCK, BLOCK)
            for hh in range(2):
                u = b * 2 + hh
                columns = head_columns(2 * role + hh)
                kf = kv_ref[rows, columns]
                state = lax.dot_general(
                    kv_ref[pl.ds((2 + b) * BLOCK, BLOCK), columns],
                    kf,
                    (((0,), (0,)), ((), ())),
                    preferred_element_type=F32,
                )
                u_ref[u * HD : (u + 1) * HD, :] = state.astype(BF16)
                total = jnp.dot(ones, kf, preferred_element_type=F32)[:1]
                tail = with_rows(tail, 2 * u, high_and_low(total))
                if u_ref is keep_ref:
                    other = b * 4 + 2 * (1 - core) + hh
                    both = [lists_ref[pl.ds(8 * i + other, 1), :] for i in (1, 0)]
                    tail = with_rows(tail, 8 + 2 * u, both)
        u_ref[STATES:, :] = tail.astype(BF16)


def key_blocks():
    gx, gy = lax.axis_index("gx"), lax.axis_index("gy")
    y, core = gy // 2, lax.rem(gy, 2)
    k = lax.rem(lax.broadcasted_iota(jnp.int32, (256, HD), 1), 16)
    back, other, b = k // 4, lax.rem(k // 2, 2), lax.rem(k, 2)
    key_x = lax.rem(gx - back * core + 4, 4)
    key_y = lax.rem(y - back * (1 - core) + 4, 4)
    key_core = core + other * (1 - 2 * core)
    return (2 * (key_x * 8 + key_y * 2 + key_core) + b).astype(F32)


def partial_kernel(*refs):
    lists, keys, outs = refs[:4], refs[4:12], list(refs[12:])
    outs[4:5] = [outs[4].at[:ROWS], outs[4].at[ROWS:]]
    core, kb = lax.rem(lax.axis_index("gy"), 2), key_blocks()
    lane = lax.broadcasted_iota(jnp.int32, (HD, 256), 0)
    col = lax.broadcasted_iota(jnp.int32, (HD, 256), 1)
    spread = jnp.where(lax.rem(lane, 16) == col // 16, 1.0, 0.0).astype(BF16)
    row = lax.broadcasted_iota(jnp.int32, (256, 256), 0)
    col = lax.broadcasted_iota(jnp.int32, (256, 256), 1)
    same = jnp.where(lax.rem(row, 16) == lax.rem(col, 16), 1.0, 0.0)
    blocks = [(d * 2 + c, b) for d in range(4) for c in range(2) for b in range(2)]
    tile_row = lax.broadcasted_iota(jnp.int32, (16, HD), 0)
    tails = [ref[STATES:, :].astype(F32) for ref in keys]
    out_tails = [jnp.zeros((16, HD), F32)] * 8
    for hh in range(2):
        listed = []
        for i, b in blocks:
            if i < 2:
                one = lists[0][pl.ds(i * 8 + b * 4 + 2 * core + hh, 1), :]
            else:
                at = 8 + 2 * (b * 2 + hh) + i % 2
                one = lists[i // 2][STATES:, :].astype(F32)[at : at + 1, :]
            listed.append(jnp.broadcast_to(one, (16, HD)))
        hit = jnp.where(jnp.concatenate(listed, axis=0) == kb, 1.0, 0.0).astype(BF16)
        mix = (jnp.dot(hit, spread, preferred_element_type=F32) * same).astype(BF16)
        for g in range(8):
            shift = hh * HD + g * 16
            pieces = [keys[i][b * 2 * HD + shift : b * 2 * HD + shift + 16, :] for i, b in blocks]
            summed = jnp.dot(mix, jnp.concatenate(pieces, axis=0), preferred_element_type=F32)
            for q, (i, b) in enumerate(blocks):
                at = b * 2 * HD + shift
                outs[i][at : at + 16, :] = summed[q * 16 : q * 16 + 16, :].astype(BF16)
        pieces = [
            jnp.where(tile_row // 2 == b * 2 + hh, tails[i], 0.0).astype(BF16) for i, b in blocks
        ]
        summed = jnp.dot(mix, jnp.concatenate(pieces, axis=0), preferred_element_type=F32)
        for q, (i, b) in enumerate(blocks):
            total = jnp.sum(summed[q * 16 : q * 16 + 8, :], axis=0, keepdims=True)
            out_tails[i] = with_rows(out_tails[i], 2 * (b * 2 + hh), high_and_low(total))
    for out_ref, tail in zip(outs, out_tails):
        out_ref[STATES:, :] = tail.astype(BF16)


def attend(q_ref, state_ref, sums_ref, at, rows, columns):
    dims = (((1,), (1,)), ((), ()))
    q = q_ref[rows, columns]
    num = lax.dot_general(q, state_ref[at, :], dims, preferred_element_type=F32)
    sums = sums_ref[at, :]
    return (num / lax.dot_general(q, sums, dims, preferred_element_type=F32)).astype(BF16)


def far_kernel(qf_ref, w_ref, *refs):
    parts, (right_ref, left_ref, state_ref, sums_ref, att_ref) = (refs[:4], refs[4:8]), refs[8:]
    core, far = lax.rem(lax.axis_index("gy"), 2), lax.rem(lax.axis_index("gz") + 4, 8)
    parts = [[*p[:2], p[2].at[side * ROWS : (side + 1) * ROWS], p[3]] for side, p in enumerate(parts)]
    for side in range(2):
        role = core if side == 0 else 1 - core
        tail = sum(p[STATES:, :].astype(F32) for p in parts[side])
        for u in range(4):
            total = sum(p[u * HD : (u + 1) * HD, :].astype(F32) for p in parts[side])
            to = pl.ds(pl.multiple_of((u // 2 * 4 + 2 * role + u % 2) * HD, HD), HD)
            state_ref[to, :] = total.astype(BF16)
            key_sum = tail[2 * u : 2 * u + 1] + tail[2 * u + 1 : 2 * u + 2]
            sums_ref[to, :] = jnp.broadcast_to(key_sum, (HD, HD)).astype(BF16)
    for h in range(4):
        at = pl.ds(pl.multiple_of((far // 4 * 4 + h) * HD, HD), HD)
        columns = slice(h * HD, (h + 1) * HD)
        att_ref[:, columns] = attend(qf_ref, state_ref, sums_ref, at, chunk_rows(far), columns)
    half = w_ref.shape[1] // 2
    right_ref[...] = jnp.dot(att_ref[...], w_ref[:, half:], preferred_element_type=F32).astype(BF16)
    left_ref[...] = jnp.dot(att_ref[...], w_ref[:, :half], preferred_element_type=F32).astype(BF16)


def project_kernel(qf_ref, w_ref, state_ref, sums_ref, *refs):
    r3_ref, l3_ref, f3_ref, e2_ref, f2_ref, e1_ref, f1_ref, own_ref, att_ref = refs
    gz = lax.axis_index("gz")
    for b in range(2):
        for h in range(4):
            at, columns = pl.ds((b * 4 + h) * HD, HD), slice(h * HD, (h + 1) * HD)
            rows = pl.ds(b * BLOCK, BLOCK)
            att_ref[rows, columns] = attend(qf_ref, state_ref, sums_ref, at, rows, columns)
    hops = (3, 5, 2, 6, 1, 7, 0)
    lhs = jnp.concatenate([att_ref[chunk_rows(lax.rem(gz + hop, 8)), :] for hop in hops], axis=0)
    half = w_ref.shape[1] // 2
    for i in range(2):
        for c in range(0, half, 512):
            out = jnp.dot(lhs, w_ref[:, i * half + c : i * half + c + 512], preferred_element_type=F32)
            cols = slice(c, c + 512)
            for n, (e_ref, f_ref) in enumerate(((None, f3_ref), (e2_ref, f2_ref), (e1_ref, f1_ref))):
                right, left = out[n * 128 : n * 128 + 64], out[n * 128 + 64 : n * 128 + 128]
                early = (right, left)[i]
                f_ref[(64, 0)[i] : (128, 64)[i], cols] = (left, right)[i]
                if e_ref is None:
                    (r3_ref, l3_ref)[i][:, cols] = early.astype(BF16)
                else:
                    e_ref[(0, 64)[i] : (64, 128)[i], cols] = early
            own_ref[:, i * half + c : i * half + c + 512] = out[384:448]


def hop_kernel(term_ref, from_left_ref, from_right_ref, right_ref, left_ref):
    right_ref[...] = (term_ref[:64, :] + from_left_ref[...].astype(F32)).astype(BF16)
    left_ref[...] = (term_ref[64:, :] + from_right_ref[...].astype(F32)).astype(BF16)


def last_kernel(own_ref, right0, left1, right1, left0, out_hbm, out_ref, sems):
    half, step = own_ref.shape[1] // 2, own_ref.shape[1] // 4
    copies = []
    for i, (a, b) in enumerate(((right0, left0), (right1, left1))):
        for c in range(0, half, step):
            cols = slice(i * half + c, i * half + c + step)
            out_ref[:, cols] = (
                own_ref[:, cols] + a[:, c : c + step].astype(F32) + b[:, c : c + step].astype(F32)
            ).astype(BF16)
            to = pl.ds(i * half + c, step)
            copies.append(
                pltpu.make_async_copy(out_ref.at[:, to], out_hbm.at[:, to], sems.at[len(copies)])
            )
            copies[-1].start()
    for copy in copies:
        copy.wait()


def per_device(queries, key_rows, values, tile_list, out_weight):
    def by_role(a, d, axes, cross=False):
        pairs = []
        for i in range(4):
            for j in range(4):
                for c in range(2):
                    to = ((i + d) % 4, j) if axes[c] == "x" else (i, (j + d) % 4)
                    pairs.append((i * 8 + j * 2 + c, to[0] * 8 + to[1] * 2 + (c ^ cross)))
        return lax.ppermute(a, ("gx", "gy"), pairs)

    to_mate = lambda a: lax.ppermute(a, "gy", [(i, i ^ 1) for i in range(8)])
    along_z = lambda a, d: lax.ppermute(a, "gz", [(i, (i + d) % 8) for i in range(8)])

    unit = jax.ShapeDtypeStruct((ROWS, HD), BF16)
    kv = jnp.concatenate([features(key_rows), values])
    keep, send, lists = call(
        states_kernel, (unit, unit, jax.ShapeDtypeStruct((16, HD), F32)), 10**9, 8
    )(kv, tile_list, to_mate(tile_list))
    keys = {(0, 0): keep}
    keys[1, 0] = by_role(keep, 1, "yx")
    keys[3, 1] = by_role(send, 3, "xy", cross=True)
    keys[3, 0] = by_role(keep, 3, "yx")
    keys[1, 1] = by_role(send, 1, "xy", cross=True)
    keys[2, 0] = by_role(keys[1, 0], 1, "yx")
    keys[2, 1] = by_role(keys[3, 1], 3, "yx")
    keys[0, 1] = to_mate(send)

    lists = [lists]
    for d in (1, 2, 3):
        lists.append(to_mate(keys[d, 0]))
    order = [(d, c) for d in range(4) for c in range(2)]
    pair = jax.ShapeDtypeStruct((2 * ROWS, HD), BF16)
    parts = call(partial_kernel, (unit,) * 4 + (pair,) + (unit,) * 2, 10**9, 16)(
        *lists, *(keys[i] for i in order)
    )
    parts = dict(zip(order[:5] + order[6:], parts))
    parts[2, 0] = by_role(parts[2, 0], 2, "xy")
    parts[2, 1] = to_mate(parts[2, 0])
    for d in (1, 3):
        parts[d, 0] = by_role(parts[d, 0], -d, "xy")
        parts[d, 1] = by_role(parts[d, 1], -d, "xy", cross=True)
    parts[0, 1] = to_mate(parts[0, 1])

    qf = features(queries)
    half = out_weight.shape[1] // 2
    piece = jax.ShapeDtypeStruct((64, half), BF16)
    heads = jax.ShapeDtypeStruct((8 * HD, HD), BF16)
    right1, left0, states, sums, _ = call(
        far_kernel,
        (piece, piece, heads, heads, jax.ShapeDtypeStruct((64, queries.shape[1]), BF16)),
        10**9,
        16,
    )(qf, out_weight, *(parts[d, c] for c in range(2) for d in range(4)))
    right1, left0 = along_z(right1, 1), along_z(left0, -1)
    term = jax.ShapeDtypeStruct((128, half), F32)
    right0, left1, f3, e2, f2, e1, f1, own, _ = call(
        project_kernel,
        (piece, piece)
        + (term,) * 5
        + (jax.ShapeDtypeStruct((64, 2 * half), F32), jax.ShapeDtypeStruct(queries.shape, BF16)),
        4 * 10**9,
        20,
    )(qf, out_weight, states, sums)
    right0, left1 = along_z(right0, 1), along_z(left1, -1)

    def hop(term, from_left, from_right):
        right, left = call(hop_kernel, (piece, piece), 10**8, 4)(term, from_left, from_right)
        return along_z(right, 1), along_z(left, -1)

    right1, left0 = hop(f3, right1, left0)
    right0, left1 = hop(e2, right0, left1)
    right1, left0 = hop(f2, right1, left0)
    right0, left1 = hop(e1, right0, left1)
    right1, left0 = hop(f1, right1, left0)
    return pl.pallas_call(
        last_kernel,
        out_shape=jax.ShapeDtypeStruct((64, 2 * half), BF16),
        out_specs=pl.BlockSpec(memory_space=pltpu.HBM),
        scratch_shapes=[pltpu.VMEM((64, 2 * half), BF16), pltpu.SemaphoreType.DMA((4,))],
        compiler_params=pltpu.CompilerParams(vmem_limit_bytes=8 << 20),
        cost_estimate=pl.CostEstimate(flops=10**8, bytes_accessed=10**6, transcendentals=0),
        name="last",
    )(own, right0, left1, right1, left0)


def solution(mesh):
    return jax.shard_map(
        per_device,
        mesh=mesh,
        in_specs=(
            P(("gx", "gy"), "gz"),
            P(("gx", "gy"), "gz"),
            P(("gx", "gy"), "gz"),
            P(("gx", "gy"), "gz", None),
            P("gz", None),
        ),
        out_specs=P(("gx", "gy", "gz"), None),
        check_vma=False,
    )
```

```python
import jax
import jax.numpy as jnp
from jax import lax
from jax.experimental import pallas as pl
from jax.experimental.pallas import tpu as pltpu
from jax.sharding import PartitionSpec as P

BLOCK = 256
HD = 128
STATES = 4 * HD
ROWS = STATES + 16
F32 = jnp.float32
BF16 = jnp.bfloat16


def call(kernel, out_shape, flops, vmem_mib):
    return pl.pallas_call(
        kernel,
        out_shape=out_shape,
        compiler_params=pltpu.CompilerParams(vmem_limit_bytes=vmem_mib << 20),
        cost_estimate=pl.CostEstimate(flops=flops, bytes_accessed=flops // 256, transcendentals=0),
    )


def features(source):
    widened = source.astype(F32)
    return jnp.where(widened > 0, widened + 1.0, jnp.exp(jnp.minimum(widened, 0.0))).astype(BF16)


def high_and_low(total):
    high = total.astype(BF16).astype(F32)
    return high, total - high


def with_rows(tail, at, rows):
    row = lax.broadcasted_iota(jnp.int32, (16, HD), 0)
    for i, one in enumerate(rows):
        tail = jnp.where(row == at + i, one, tail)
    return tail


def head_columns(h):
    return pl.ds(pl.multiple_of(h * HD, HD), HD)


def chunk_rows(j):
    return pl.ds(pl.multiple_of(j * 64, 64), 64)


def states_kernel(kv_ref, own_ref, mate_ref, keep_ref, send_ref, lists_ref):
    core = lax.rem(lax.axis_index("gy"), 2)
    ones = jnp.ones((16, BLOCK), BF16)
    entry = lax.broadcasted_iota(jnp.int32, (8, HD), 0)
    lane = lax.broadcasted_iota(jnp.int32, (8, HD), 1)
    repeat = jnp.where(lane // 16 == entry, 1.0, 0.0).astype(BF16)
    for i, list_ref in enumerate((own_ref, mate_ref)):
        for b in range(2):
            listed = list_ref[b].astype(F32).astype(BF16)
            at = i * 8 + b * 4
            lists_ref[at : at + 4, :] = jnp.dot(listed, repeat, preferred_element_type=F32)
    for u_ref, role in ((keep_ref, core), (send_ref, 1 - core)):
        tail = jnp.zeros((16, HD), F32)
        for b in range(2):
            rows = pl.ds(b * BLOCK, BLOCK)
            for hh in range(2):
                u = b * 2 + hh
                columns = head_columns(2 * role + hh)
                kf = kv_ref[rows, columns]
                state = lax.dot_general(
                    kv_ref[pl.ds((2 + b) * BLOCK, BLOCK), columns],
                    kf,
                    (((0,), (0,)), ((), ())),
                    preferred_element_type=F32,
                )
                u_ref[u * HD : (u + 1) * HD, :] = state.astype(BF16)
                total = jnp.dot(ones, kf, preferred_element_type=F32)[:1]
                tail = with_rows(tail, 2 * u, high_and_low(total))
                if u_ref is keep_ref:
                    other = b * 4 + 2 * (1 - core) + hh
                    both = [lists_ref[pl.ds(8 * i + other, 1), :] for i in (1, 0)]
                    tail = with_rows(tail, 8 + 2 * u, both)
        u_ref[STATES:, :] = tail.astype(BF16)


def key_blocks():
    gx, gy = lax.axis_index("gx"), lax.axis_index("gy")
    y, core = gy // 2, lax.rem(gy, 2)
    k = lax.rem(lax.broadcasted_iota(jnp.int32, (256, HD), 1), 16)
    back, other, b = k // 4, lax.rem(k // 2, 2), lax.rem(k, 2)
    key_x = lax.rem(gx - back * core + 4, 4)
    key_y = lax.rem(y - back * (1 - core) + 4, 4)
    key_core = core + other * (1 - 2 * core)
    return (2 * (key_x * 8 + key_y * 2 + key_core) + b).astype(F32)


def partial_kernel(*refs):
    lists, keys, outs = refs[:4], refs[4:12], list(refs[12:])
    outs[4:5] = [outs[4].at[:ROWS], outs[4].at[ROWS:]]
    core, kb = lax.rem(lax.axis_index("gy"), 2), key_blocks()
    lane = lax.broadcasted_iota(jnp.int32, (HD, 256), 0)
    col = lax.broadcasted_iota(jnp.int32, (HD, 256), 1)
    spread = jnp.where(lax.rem(lane, 16) == col // 16, 1.0, 0.0).astype(BF16)
    row = lax.broadcasted_iota(jnp.int32, (256, 256), 0)
    col = lax.broadcasted_iota(jnp.int32, (256, 256), 1)
    same = jnp.where(lax.rem(row, 16) == lax.rem(col, 16), 1.0, 0.0)
    blocks = [(d * 2 + c, b) for d in range(4) for c in range(2) for b in range(2)]
    tile_row = lax.broadcasted_iota(jnp.int32, (16, HD), 0)
    tails = [ref[STATES:, :].astype(F32) for ref in keys]
    out_tails = [jnp.zeros((16, HD), F32)] * 8
    for hh in range(2):
        listed = []
        for i, b in blocks:
            if i < 2:
                one = lists[0][pl.ds(i * 8 + b * 4 + 2 * core + hh, 1), :]
            else:
                at = 8 + 2 * (b * 2 + hh) + i % 2
                one = lists[i // 2][STATES:, :].astype(F32)[at : at + 1, :]
            listed.append(jnp.broadcast_to(one, (16, HD)))
        hit = jnp.where(jnp.concatenate(listed, axis=0) == kb, 1.0, 0.0).astype(BF16)
        mix = (jnp.dot(hit, spread, preferred_element_type=F32) * same).astype(BF16)
        for g in range(8):
            shift = hh * HD + g * 16
            pieces = [keys[i][b * 2 * HD + shift : b * 2 * HD + shift + 16, :] for i, b in blocks]
            summed = jnp.dot(mix, jnp.concatenate(pieces, axis=0), preferred_element_type=F32)
            for q, (i, b) in enumerate(blocks):
                at = b * 2 * HD + shift
                outs[i][at : at + 16, :] = summed[q * 16 : q * 16 + 16, :].astype(BF16)
        pieces = [
            jnp.where(tile_row // 2 == b * 2 + hh, tails[i], 0.0).astype(BF16) for i, b in blocks
        ]
        summed = jnp.dot(mix, jnp.concatenate(pieces, axis=0), preferred_element_type=F32)
        for q, (i, b) in enumerate(blocks):
            total = jnp.sum(summed[q * 16 : q * 16 + 8, :], axis=0, keepdims=True)
            out_tails[i] = with_rows(out_tails[i], 2 * (b * 2 + hh), high_and_low(total))
    for out_ref, tail in zip(outs, out_tails):
        out_ref[STATES:, :] = tail.astype(BF16)


def attend(q_ref, state_ref, sums_ref, at, rows, columns):
    dims = (((1,), (1,)), ((), ()))
    q = q_ref[rows, columns]
    num = lax.dot_general(q, state_ref[at, :], dims, preferred_element_type=F32)
    sums = sums_ref[at, :]
    return (num / lax.dot_general(q, sums, dims, preferred_element_type=F32)).astype(BF16)


def far_kernel(qf_ref, w_ref, *refs):
    parts, (right_ref, left_ref, state_ref, sums_ref, att_ref) = (refs[:4], refs[4:8]), refs[8:]
    core, far = lax.rem(lax.axis_index("gy"), 2), lax.rem(lax.axis_index("gz") + 4, 8)
    parts = [[*p[:2], p[2].at[side * ROWS : (side + 1) * ROWS], p[3]] for side, p in enumerate(parts)]
    for side in range(2):
        role = core if side == 0 else 1 - core
        tail = sum(p[STATES:, :].astype(F32) for p in parts[side])
        for u in range(4):
            total = sum(p[u * HD : (u + 1) * HD, :].astype(F32) for p in parts[side])
            to = pl.ds(pl.multiple_of((u // 2 * 4 + 2 * role + u % 2) * HD, HD), HD)
            state_ref[to, :] = total.astype(BF16)
            key_sum = tail[2 * u : 2 * u + 1] + tail[2 * u + 1 : 2 * u + 2]
            sums_ref[to, :] = jnp.broadcast_to(key_sum, (HD, HD)).astype(BF16)
    for h in range(4):
        at = pl.ds(pl.multiple_of((far // 4 * 4 + h) * HD, HD), HD)
        columns = slice(h * HD, (h + 1) * HD)
        att_ref[:, columns] = attend(qf_ref, state_ref, sums_ref, at, chunk_rows(far), columns)
    half = w_ref.shape[1] // 2
    right_ref[...] = jnp.dot(att_ref[...], w_ref[:, half:], preferred_element_type=F32).astype(BF16)
    left_ref[...] = jnp.dot(att_ref[...], w_ref[:, :half], preferred_element_type=F32).astype(BF16)


def project_kernel(qf_ref, w_ref, state_ref, sums_ref, *refs):
    r3_ref, l3_ref, f3_ref, e2_ref, f2_ref, e1_ref, f1_ref, own_ref, att_ref = refs
    gz = lax.axis_index("gz")
    for b in range(2):
        for h in range(4):
            at, columns = pl.ds((b * 4 + h) * HD, HD), slice(h * HD, (h + 1) * HD)
            rows = pl.ds(b * BLOCK, BLOCK)
            att_ref[rows, columns] = attend(qf_ref, state_ref, sums_ref, at, rows, columns)
    hops = (3, 5, 2, 6, 1, 7, 0)
    lhs = jnp.concatenate([att_ref[chunk_rows(lax.rem(gz + hop, 8)), :] for hop in hops], axis=0)
    half = w_ref.shape[1] // 2
    for i in range(2):
        for c in range(0, half, 512):
            out = jnp.dot(lhs, w_ref[:, i * half + c : i * half + c + 512], preferred_element_type=F32)
            cols = slice(c, c + 512)
            for n, (e_ref, f_ref) in enumerate(((None, f3_ref), (e2_ref, f2_ref), (e1_ref, f1_ref))):
                right, left = out[n * 128 : n * 128 + 64], out[n * 128 + 64 : n * 128 + 128]
                early = (right, left)[i]
                f_ref[(64, 0)[i] : (128, 64)[i], cols] = (left, right)[i]
                if e_ref is None:
                    (r3_ref, l3_ref)[i][:, cols] = early.astype(BF16)
                else:
                    e_ref[(0, 64)[i] : (64, 128)[i], cols] = early
            own_ref[:, i * half + c : i * half + c + 512] = out[384:448]


def hop_kernel(term_ref, from_left_ref, from_right_ref, right_ref, left_ref):
    right_ref[...] = (term_ref[:64, :] + from_left_ref[...].astype(F32)).astype(BF16)
    left_ref[...] = (term_ref[64:, :] + from_right_ref[...].astype(F32)).astype(BF16)


def last_kernel(own_ref, right0, left1, right1, left0, out_hbm, out_ref, sems):
    half, step = own_ref.shape[1] // 2, own_ref.shape[1] // 4
    copies = []
    for i, (a, b) in enumerate(((right0, left0), (right1, left1))):
        for c in range(0, half, step):
            cols = slice(i * half + c, i * half + c + step)
            out_ref[:, cols] = (
                own_ref[:, cols] + a[:, c : c + step].astype(F32) + b[:, c : c + step].astype(F32)
            ).astype(BF16)
            to = pl.ds(i * half + c, step)
            copies.append(
                pltpu.make_async_copy(out_ref.at[:, to], out_hbm.at[:, to], sems.at[len(copies)])
            )
            copies[-1].start()
    for copy in copies:
        copy.wait()


def per_device(queries, key_rows, values, tile_list, out_weight):
    def by_role(a, d, axes, cross=False):
        pairs = []
        for i in range(4):
            for j in range(4):
                for c in range(2):
                    to = ((i + d) % 4, j) if axes[c] == "x" else (i, (j + d) % 4)
                    pairs.append((i * 8 + j * 2 + c, to[0] * 8 + to[1] * 2 + (c ^ cross)))
        return lax.ppermute(a, ("gx", "gy"), pairs)

    to_mate = lambda a: lax.ppermute(a, "gy", [(i, i ^ 1) for i in range(8)])
    along_z = lambda a, d: lax.ppermute(a, "gz", [(i, (i + d) % 8) for i in range(8)])

    unit = jax.ShapeDtypeStruct((ROWS, HD), BF16)
    kv = jnp.concatenate([features(key_rows), values])
    keep, send, lists = call(
        states_kernel, (unit, unit, jax.ShapeDtypeStruct((16, HD), F32)), 10**9, 8
    )(kv, tile_list, to_mate(tile_list))
    keys = {(0, 0): keep}
    keys[1, 0] = by_role(keep, 1, "yx")
    keys[3, 1] = by_role(send, 3, "xy", cross=True)
    keys[3, 0] = by_role(keep, 3, "yx")
    keys[1, 1] = by_role(send, 1, "xy", cross=True)
    keys[2, 0] = by_role(keys[1, 0], 1, "yx")
    keys[2, 1] = by_role(keys[3, 1], 3, "yx")
    keys[0, 1] = to_mate(send)

    lists = [lists]
    for d in (1, 2, 3):
        lists.append(to_mate(keys[d, 0]))
    order = [(d, c) for d in range(4) for c in range(2)]
    pair = jax.ShapeDtypeStruct((2 * ROWS, HD), BF16)
    parts = call(partial_kernel, (unit,) * 4 + (pair,) + (unit,) * 2, 10**9, 16)(
        *lists, *(keys[i] for i in order)
    )
    parts = dict(zip(order[:5] + order[6:], parts))
    parts[2, 0] = by_role(parts[2, 0], 2, "xy")
    parts[2, 1] = to_mate(parts[2, 0])
    for d in (1, 3):
        parts[d, 0] = by_role(parts[d, 0], -d, "xy")
        parts[d, 1] = by_role(parts[d, 1], -d, "xy", cross=True)
    parts[0, 1] = to_mate(parts[0, 1])

    qf = features(queries)
    half = out_weight.shape[1] // 2
    piece = jax.ShapeDtypeStruct((64, half), BF16)
    heads = jax.ShapeDtypeStruct((8 * HD, HD), BF16)
    right1, left0, states, sums, _ = call(
        far_kernel,
        (piece, piece, heads, heads, jax.ShapeDtypeStruct((64, queries.shape[1]), BF16)),
        10**9,
        16,
    )(qf, out_weight, *(parts[d, c] for c in range(2) for d in range(4)))
    right1 = along_z(right1, 1)
    left0 = along_z(left0, -1)
    term = jax.ShapeDtypeStruct((128, half), F32)
    right0, left1, f3, e2, f2, e1, f1, own, _ = call(
        project_kernel,
        (piece, piece)
        + (term,) * 5
        + (jax.ShapeDtypeStruct((64, 2 * half), F32), jax.ShapeDtypeStruct(queries.shape, BF16)),
        4 * 10**9,
        20,
    )(qf, out_weight, states, sums)
    right0, left1 = along_z(right0, 1), along_z(left1, -1)

    def hop(term, from_left, from_right):
        right, left = call(hop_kernel, (piece, piece), 10**8, 4)(term, from_left, from_right)
        right = along_z(right, 1)
        left = along_z(left, -1)
        return right, left

    right1, left0 = hop(f3, right1, left0)
    right0, left1 = hop(e2, right0, left1)
    right1, left0 = hop(f2, right1, left0)
    right0, left1 = hop(e1, right0, left1)
    right1, left0 = hop(f1, right1, left0)
    return pl.pallas_call(
        last_kernel,
        out_shape=jax.ShapeDtypeStruct((64, 2 * half), BF16),
        out_specs=pl.BlockSpec(memory_space=pltpu.HBM),
        scratch_shapes=[pltpu.VMEM((64, 2 * half), BF16), pltpu.SemaphoreType.DMA((4,))],
        compiler_params=pltpu.CompilerParams(vmem_limit_bytes=8 << 20),
        cost_estimate=pl.CostEstimate(flops=10**8, bytes_accessed=10**6, transcendentals=0),
        name="last",
    )(own, right0, left1, right1, left0)


def solution(mesh):
    return jax.shard_map(
        per_device,
        mesh=mesh,
        in_specs=(
            P(("gx", "gy"), "gz"),
            P(("gx", "gy"), "gz"),
            P(("gx", "gy"), "gz"),
            P(("gx", "gy"), "gz", None),
            P("gz", None),
        ),
        out_specs=P(("gx", "gy", "gz"), None),
        check_vma=False,
    )
```

```python
import jax
import jax.numpy as jnp
from jax import lax
from jax.experimental import pallas as pl
from jax.experimental.pallas import tpu as pltpu
from jax.sharding import PartitionSpec as P

BLOCK = 256
HD = 128
STATES = 4 * HD
ROWS = STATES + 16
F32 = jnp.float32
BF16 = jnp.bfloat16


def call(kernel, out_shape, flops, vmem_mib):
    return pl.pallas_call(
        kernel,
        out_shape=out_shape,
        compiler_params=pltpu.CompilerParams(vmem_limit_bytes=vmem_mib << 20),
        cost_estimate=pl.CostEstimate(flops=flops, bytes_accessed=flops // 256, transcendentals=0),
    )


def features(source):
    widened = source.astype(F32)
    return jnp.where(widened > 0, widened + 1.0, jnp.exp(jnp.minimum(widened, 0.0))).astype(BF16)


def high_and_low(total):
    high = total.astype(BF16).astype(F32)
    return high, total - high


def with_rows(tail, at, rows):
    row = lax.broadcasted_iota(jnp.int32, (16, HD), 0)
    for i, one in enumerate(rows):
        tail = jnp.where(row == at + i, one, tail)
    return tail


def head_columns(h):
    return pl.ds(pl.multiple_of(h * HD, HD), HD)


def chunk_rows(j):
    return pl.ds(pl.multiple_of(j * 64, 64), 64)


def states_kernel(kv_ref, own_ref, mate_ref, keep_ref, send_ref, lists_ref):
    core = lax.rem(lax.axis_index("gy"), 2)
    ones = jnp.ones((16, BLOCK), BF16)
    entry = lax.broadcasted_iota(jnp.int32, (8, HD), 0)
    lane = lax.broadcasted_iota(jnp.int32, (8, HD), 1)
    repeat = jnp.where(lane // 16 == entry, 1.0, 0.0).astype(BF16)
    for i, list_ref in enumerate((own_ref, mate_ref)):
        for b in range(2):
            listed = list_ref[b].astype(F32).astype(BF16)
            at = i * 8 + b * 4
            lists_ref[at : at + 4, :] = jnp.dot(listed, repeat, preferred_element_type=F32)
    for u_ref, role in ((keep_ref, core), (send_ref, 1 - core)):
        tail = jnp.zeros((16, HD), F32)
        for b in range(2):
            rows = pl.ds(b * BLOCK, BLOCK)
            for hh in range(2):
                u = b * 2 + hh
                columns = head_columns(2 * role + hh)
                kf = kv_ref[rows, columns]
                state = lax.dot_general(
                    kv_ref[pl.ds((2 + b) * BLOCK, BLOCK), columns],
                    kf,
                    (((0,), (0,)), ((), ())),
                    preferred_element_type=F32,
                )
                u_ref[u * HD : (u + 1) * HD, :] = state.astype(BF16)
                total = jnp.dot(ones, kf, preferred_element_type=F32)[:1]
                tail = with_rows(tail, 2 * u, high_and_low(total))
                if u_ref is keep_ref:
                    other = b * 4 + 2 * (1 - core) + hh
                    both = [lists_ref[pl.ds(8 * i + other, 1), :] for i in (1, 0)]
                    tail = with_rows(tail, 8 + 2 * u, both)
        u_ref[STATES:, :] = tail.astype(BF16)


def key_blocks():
    gx, gy = lax.axis_index("gx"), lax.axis_index("gy")
    y, core = gy // 2, lax.rem(gy, 2)
    k = lax.rem(lax.broadcasted_iota(jnp.int32, (256, HD), 1), 16)
    back, other, b = k // 4, lax.rem(k // 2, 2), lax.rem(k, 2)
    key_x = lax.rem(gx - back * core + 4, 4)
    key_y = lax.rem(y - back * (1 - core) + 4, 4)
    key_core = core + other * (1 - 2 * core)
    return (2 * (key_x * 8 + key_y * 2 + key_core) + b).astype(F32)


def partial_kernel(*refs):
    lists, keys, outs = refs[:4], refs[4:12], list(refs[12:])
    outs[4:5] = [outs[4].at[:ROWS], outs[4].at[ROWS:]]
    core, kb = lax.rem(lax.axis_index("gy"), 2), key_blocks()
    lane = lax.broadcasted_iota(jnp.int32, (HD, 256), 0)
    col = lax.broadcasted_iota(jnp.int32, (HD, 256), 1)
    spread = jnp.where(lax.rem(lane, 16) == col // 16, 1.0, 0.0).astype(BF16)
    row = lax.broadcasted_iota(jnp.int32, (256, 256), 0)
    col = lax.broadcasted_iota(jnp.int32, (256, 256), 1)
    same = jnp.where(lax.rem(row, 16) == lax.rem(col, 16), 1.0, 0.0)
    blocks = [(d * 2 + c, b) for d in range(4) for c in range(2) for b in range(2)]
    tile_row = lax.broadcasted_iota(jnp.int32, (16, HD), 0)
    tails = [ref[STATES:, :].astype(F32) for ref in keys]
    out_tails = [jnp.zeros((16, HD), F32)] * 8
    for hh in range(2):
        listed = []
        for i, b in blocks:
            if i < 2:
                one = lists[0][pl.ds(i * 8 + b * 4 + 2 * core + hh, 1), :]
            else:
                at = 8 + 2 * (b * 2 + hh) + i % 2
                one = lists[i // 2][STATES:, :].astype(F32)[at : at + 1, :]
            listed.append(jnp.broadcast_to(one, (16, HD)))
        hit = jnp.where(jnp.concatenate(listed, axis=0) == kb, 1.0, 0.0).astype(BF16)
        mix = (jnp.dot(hit, spread, preferred_element_type=F32) * same).astype(BF16)
        for g in range(8):
            shift = hh * HD + g * 16
            pieces = [keys[i][b * 2 * HD + shift : b * 2 * HD + shift + 16, :] for i, b in blocks]
            summed = jnp.dot(mix, jnp.concatenate(pieces, axis=0), preferred_element_type=F32)
            for q, (i, b) in enumerate(blocks):
                at = b * 2 * HD + shift
                outs[i][at : at + 16, :] = summed[q * 16 : q * 16 + 16, :].astype(BF16)
        pieces = [
            jnp.where(tile_row // 2 == b * 2 + hh, tails[i], 0.0).astype(BF16) for i, b in blocks
        ]
        summed = jnp.dot(mix, jnp.concatenate(pieces, axis=0), preferred_element_type=F32)
        for q, (i, b) in enumerate(blocks):
            total = jnp.sum(summed[q * 16 : q * 16 + 8, :], axis=0, keepdims=True)
            out_tails[i] = with_rows(out_tails[i], 2 * (b * 2 + hh), high_and_low(total))
    for out_ref, tail in zip(outs, out_tails):
        out_ref[STATES:, :] = tail.astype(BF16)


def attend(q_ref, state_ref, sums_ref, at, rows, columns):
    dims = (((1,), (1,)), ((), ()))
    q = q_ref[rows, columns]
    num = lax.dot_general(q, state_ref[at, :], dims, preferred_element_type=F32)
    sums = sums_ref[at, :]
    return (num / lax.dot_general(q, sums, dims, preferred_element_type=F32)).astype(BF16)


def both_sides(refs):
    sides = (refs[:4], refs[4:8])
    return [[*p[:2], p[2].at[side * ROWS : (side + 1) * ROWS], p[3]] for side, p in enumerate(sides)]


def far_kernel(qf_ref, w_ref, *refs):
    parts, (right_ref, left_ref, state_ref, sums_ref, att_ref) = both_sides(refs[:8]), refs[8:]
    core, far = lax.rem(lax.axis_index("gy"), 2), lax.rem(lax.axis_index("gz") + 4, 8)
    block = far // 4
    for side in range(2):
        role = core if side == 0 else 1 - core
        tail = sum(p[STATES:, :].astype(F32) for p in parts[side])
        for hh in range(2):
            unit = pl.ds(pl.multiple_of((block * 2 + hh) * HD, HD), HD)
            total = sum(p[unit, :].astype(F32) for p in parts[side])
            to = pl.ds(pl.multiple_of((2 * role + hh) * HD, HD), HD)
            state_ref[to, :] = total.astype(BF16)
            first, second = (tail[2 * u : 2 * u + 1] + tail[2 * u + 1 : 2 * u + 2] for u in (hh, 2 + hh))
            key_sum = jnp.where(block == 0, first, second)
            sums_ref[to, :] = jnp.broadcast_to(key_sum, (HD, HD)).astype(BF16)
    for h in range(4):
        at, columns = pl.ds(h * HD, HD), slice(h * HD, (h + 1) * HD)
        att_ref[:, columns] = attend(qf_ref, state_ref, sums_ref, at, chunk_rows(far), columns)
    half = w_ref.shape[1] // 2
    right_ref[...] = jnp.dot(att_ref[...], w_ref[:, half:], preferred_element_type=F32).astype(BF16)
    left_ref[...] = jnp.dot(att_ref[...], w_ref[:, :half], preferred_element_type=F32).astype(BF16)


def project_kernel(qf_ref, w_ref, far_ref, *refs):
    parts = both_sides(refs[:8])
    r3_ref, l3_ref, f3_ref, e2_ref, f2_ref, e1_ref, f1_ref, own_ref = refs[8:16]
    att_ref, state_ref, sums_ref = refs[16:]
    gz, core = lax.axis_index("gz"), lax.rem(lax.axis_index("gy"), 2)
    for side in range(2):
        role = core if side == 0 else 1 - core
        tail = sum(p[STATES:, :].astype(F32) for p in parts[side])
        for u in range(4):
            total = sum(p[u * HD : (u + 1) * HD, :].astype(F32) for p in parts[side])
            to = pl.ds(pl.multiple_of((u // 2 * 4 + 2 * role + u % 2) * HD, HD), HD)
            state_ref[to, :] = total.astype(BF16)
            key_sum = tail[2 * u : 2 * u + 1] + tail[2 * u + 1 : 2 * u + 2]
            sums_ref[to, :] = jnp.broadcast_to(key_sum, (HD, HD)).astype(BF16)
    for b in range(2):
        for h in range(4):
            at, columns = pl.ds((b * 4 + h) * HD, HD), slice(h * HD, (h + 1) * HD)
            rows = pl.ds(b * BLOCK, BLOCK)
            att_ref[rows, columns] = attend(qf_ref, state_ref, sums_ref, at, rows, columns)
    hops = (3, 5, 2, 6, 1, 7, 0)
    lhs = jnp.concatenate([att_ref[chunk_rows(lax.rem(gz + hop, 8)), :] for hop in hops], axis=0)
    half = w_ref.shape[1] // 2
    for i in range(2):
        for c in range(0, half, 512):
            out = jnp.dot(lhs, w_ref[:, i * half + c : i * half + c + 512], preferred_element_type=F32)
            cols = slice(c, c + 512)
            for n, (e_ref, f_ref) in enumerate(((None, f3_ref), (e2_ref, f2_ref), (e1_ref, f1_ref))):
                right, left = out[n * 128 : n * 128 + 64], out[n * 128 + 64 : n * 128 + 128]
                early = (right, left)[i]
                f_ref[(64, 0)[i] : (128, 64)[i], cols] = (left, right)[i]
                if e_ref is None:
                    (r3_ref, l3_ref)[i][:, cols] = early.astype(BF16)
                else:
                    e_ref[(0, 64)[i] : (64, 128)[i], cols] = early
            own_ref[:, i * half + c : i * half + c + 512] = out[384:448]


def hop_kernel(term_ref, from_left_ref, from_right_ref, right_ref, left_ref):
    right_ref[...] = (term_ref[:64, :] + from_left_ref[...].astype(F32)).astype(BF16)
    left_ref[...] = (term_ref[64:, :] + from_right_ref[...].astype(F32)).astype(BF16)


def last_kernel(own_ref, right0, left1, right1, left0, out_hbm, out_ref, sems):
    half, step = own_ref.shape[1] // 2, own_ref.shape[1] // 4
    copies = []
    for i, (a, b) in enumerate(((right0, left0), (right1, left1))):
        for c in range(0, half, step):
            cols = slice(i * half + c, i * half + c + step)
            out_ref[:, cols] = (
                own_ref[:, cols] + a[:, c : c + step].astype(F32) + b[:, c : c + step].astype(F32)
            ).astype(BF16)
            to = pl.ds(i * half + c, step)
            copies.append(
                pltpu.make_async_copy(out_ref.at[:, to], out_hbm.at[:, to], sems.at[len(copies)])
            )
            copies[-1].start()
    for copy in copies:
        copy.wait()


def per_device(queries, key_rows, values, tile_list, out_weight):
    def by_role(a, d, axes, cross=False):
        pairs = []
        for i in range(4):
            for j in range(4):
                for c in range(2):
                    to = ((i + d) % 4, j) if axes[c] == "x" else (i, (j + d) % 4)
                    pairs.append((i * 8 + j * 2 + c, to[0] * 8 + to[1] * 2 + (c ^ cross)))
        return lax.ppermute(a, ("gx", "gy"), pairs)

    to_mate = lambda a: lax.ppermute(a, "gy", [(i, i ^ 1) for i in range(8)])
    along_z = lambda a, d: lax.ppermute(a, "gz", [(i, (i + d) % 8) for i in range(8)])

    unit = jax.ShapeDtypeStruct((ROWS, HD), BF16)
    kv = jnp.concatenate([features(key_rows), values])
    keep, send, lists = call(
        states_kernel, (unit, unit, jax.ShapeDtypeStruct((16, HD), F32)), 10**9, 8
    )(kv, tile_list, to_mate(tile_list))
    keys = {(0, 0): keep}
    keys[1, 0] = by_role(keep, 1, "yx")
    keys[3, 1] = by_role(send, 3, "xy", cross=True)
    keys[3, 0] = by_role(keep, 3, "yx")
    keys[1, 1] = by_role(send, 1, "xy", cross=True)
    keys[2, 0] = by_role(keys[1, 0], 1, "yx")
    keys[2, 1] = by_role(keys[3, 1], 3, "yx")
    keys[0, 1] = to_mate(send)

    lists = [lists]
    for d in (1, 2, 3):
        lists.append(to_mate(keys[d, 0]))
    order = [(d, c) for d in range(4) for c in range(2)]
    pair = jax.ShapeDtypeStruct((2 * ROWS, HD), BF16)
    parts = call(partial_kernel, (unit,) * 4 + (pair,) + (unit,) * 2, 10**9, 16)(
        *lists, *(keys[i] for i in order)
    )
    parts = dict(zip(order[:5] + order[6:], parts))
    parts[2, 0] = by_role(parts[2, 0], 2, "xy")
    parts[2, 1] = to_mate(parts[2, 0])
    for d in (1, 3):
        parts[d, 0] = by_role(parts[d, 0], -d, "xy")
        parts[d, 1] = by_role(parts[d, 1], -d, "xy", cross=True)
    parts[0, 1] = to_mate(parts[0, 1])

    qf = features(queries)
    half = out_weight.shape[1] // 2
    piece = jax.ShapeDtypeStruct((64, half), BF16)
    heads = jax.ShapeDtypeStruct((8 * HD, HD), BF16)
    few = jax.ShapeDtypeStruct((4 * HD, HD), BF16)
    summed = [parts[d, c] for c in range(2) for d in range(4)]
    right1, left0, states, _, _ = call(
        far_kernel,
        (piece, piece, few, few, jax.ShapeDtypeStruct((64, queries.shape[1]), BF16)),
        10**9,
        16,
    )(qf, out_weight, *summed)
    right1 = along_z(right1, 1)
    left0 = along_z(left0, -1)
    term = jax.ShapeDtypeStruct((128, half), F32)
    right0, left1, f3, e2, f2, e1, f1, own, *_ = call(
        project_kernel,
        (piece, piece)
        + (term,) * 5
        + (jax.ShapeDtypeStruct((64, 2 * half), F32), jax.ShapeDtypeStruct(queries.shape, BF16), heads, heads),
        4 * 10**9,
        20,
    )(qf, out_weight, states, *summed)
    right0, left1 = along_z(right0, 1), along_z(left1, -1)

    def hop(term, from_left, from_right):
        right, left = call(hop_kernel, (piece, piece), 10**8, 4)(term, from_left, from_right)
        right = along_z(right, 1)
        left = along_z(left, -1)
        return right, left

    right1, left0 = hop(f3, right1, left0)
    right0, left1 = hop(e2, right0, left1)
    right1, left0 = hop(f2, right1, left0)
    right0, left1 = hop(e1, right0, left1)
    right1, left0 = hop(f1, right1, left0)
    return pl.pallas_call(
        last_kernel,
        out_shape=jax.ShapeDtypeStruct((64, 2 * half), BF16),
        out_specs=pl.BlockSpec(memory_space=pltpu.HBM),
        scratch_shapes=[pltpu.VMEM((64, 2 * half), BF16), pltpu.SemaphoreType.DMA((4,))],
        compiler_params=pltpu.CompilerParams(vmem_limit_bytes=8 << 20),
        cost_estimate=pl.CostEstimate(flops=10**8, bytes_accessed=10**6, transcendentals=0),
        name="last",
    )(own, right0, left1, right1, left0)


def solution(mesh):
    return jax.shard_map(
        per_device,
        mesh=mesh,
        in_specs=(
            P(("gx", "gy"), "gz"),
            P(("gx", "gy"), "gz"),
            P(("gx", "gy"), "gz"),
            P(("gx", "gy"), "gz", None),
            P("gz", None),
        ),
        out_specs=P(("gx", "gy", "gz"), None),
        check_vma=False,
    )
```
